32 devices in a mesh: gx: 8 (over z, x), gy: 4 (over y, core).
Axes of the slice: x: 2, y: 2, z: 4, core: 2. Of those that a mesh axis runs over, the one named last changes fastest.
Arguments:
- probe_seeds: int32 [4], replicated, may hold values from 0 to 1048575
- damping: float32 [512, 1024], P('gx', 'gy'), may hold values from 0.2 to 1
- coupling_x: float32 [512, 1024], P('gx', 'gy'), may hold values from 0.05 to 0.5
- coupling_y: float32 [512, 1024], P('gx', 'gy'), may hold values from 0.05 to 0.5
- sensor_count: int32 [8, 4], P('gx', 'gy'), may hold values from 1 to 256, as said below
- sensor_cells: int32 [8, 4, 256], P('gx', 'gy'), may hold values from 0 to 16383
- obs_weight: float32 [8, 4, 256, 256], P('gx', 'gy'), as said below
Outputs:
- solution: float32 [4, 512, 1024], P(None, 'gx', 'gy')
- trace_estimate: float32 [], replicated
The draws below stay inside these ranges and needn't reach their ends.
Inputs may be any that keep to these rules, and one draw needn't show every extreme that they name: `sensor_count`: at most 256, and some block has exactly 256 in every draw; blocks near a few cluster centres are far busier than the rest. `sensor_cells`: cells within the block, numbered row by row. `obs_weight`: each block's matrix is symmetric positive definite.
All inputs are finite; a program needn't handle non-finite values.
Results may differ from the reference program's by a relative error of at most 0.0003.
Values sent between devices are 32-bit elements; how exact they have to be, the bound alone decides.
No kernel may reach another device: no remote copies, remote signals or barrier semaphores. Data moves between devices by JAX's collectives and lax.ppermute only.
A program may use at most 64 MiB of HBM per device.

```python
import math
import jax
import jax.numpy as jnp
from jax import lax

PROBES = 4
CX = 64
CY = 256
SMAX = 256
BX = 8
BY = 4
NX = 512
NY = 1024


def draw_sensor_count(key, part):
    key_base, key_rows, key_cols = jax.random.split(jax.random.fold_in(key, 101), 3)
    base = jax.random.randint(key_base, (BX, BY), 1, SMAX // 4 + 1)
    centre_rows = jax.random.randint(key_rows, (3,), 0, BX)
    centre_cols = jax.random.randint(key_cols, (3,), 0, BY)
    block_rows = jnp.arange(BX, dtype=jnp.int32)[:, None, None]
    block_cols = jnp.arange(BY, dtype=jnp.int32)[None, :, None]
    apart_rows = jnp.abs(block_rows - centre_rows[None, None, :])
    apart_rows = jnp.minimum(apart_rows, BX - apart_rows)
    apart_cols = jnp.abs(block_cols - centre_cols[None, None, :])
    apart_cols = jnp.minimum(apart_cols, BY - apart_cols)
    distance = apart_rows + apart_cols
    centre = jnp.any(distance == 0, axis=2)
    nearby = jnp.any(distance <= 1, axis=2)
    counts = jnp.where(nearby, jnp.maximum(base, SMAX // 2), base)
    return jnp.where(centre, SMAX, counts).astype(jnp.int32)


def draw_obs_weight(key, part):
    key_mix, key_diag = jax.random.split(jax.random.fold_in(key, 202))
    normal_part = jax.random.normal(key_mix, (BX, BY, SMAX, SMAX), jnp.float32)
    product = jnp.einsum('abij,abkj->abik', normal_part, normal_part) / (2.0 * math.sqrt(SMAX))
    product = 0.5 * (product + jnp.swapaxes(product, 2, 3))
    diagonal = jnp.exp(jax.random.uniform(key_diag, (BX, BY, SMAX), jnp.float32, 0.0, math.log(10.0)))
    return (product + diagonal[..., None] * jnp.eye(SMAX, dtype=jnp.float32)).astype(jnp.float32)


def touch_ends(result, own_key, smallest, top_value):
    index_at = [jax.random.randint(jax.random.fold_in(own_key, axis), (), 0, length) for axis, length in enumerate(result.shape)]
    widest = result.shape.index(max(result.shape))
    next_to = index_at[:widest] + [(index_at[widest] + 1) % result.shape[widest]] + index_at[widest + 1:]
    return result.at[tuple(index_at)].set(smallest).at[tuple(next_to)].set(top_value)


def shard_levels(key, shape, shards, least, high):
    def one(axis_at, parts):
        heights = jax.random.uniform(jax.random.fold_in(jax.random.fold_in(key, 6), axis_at), (parts,), jnp.float32, least / len(shards), high / len(shards))
        return jnp.repeat(jnp.exp(heights), shape[axis_at] // parts).reshape((-1,) + (1,) * (len(shape) - axis_at - 1))

    gain = one(*shards[0])
    for cut in shards[1:]:
        gain = gain * one(*cut)
    return gain


def setup_inputs(seed: int = 0) -> dict:
    key_list = jax.random.split(jax.random.key(seed), 8)
    probe_seeds = touch_ends(jax.random.randint(key_list[0], (PROBES,), 0, 1048576), jax.random.fold_in(key_list[0], 1), 0, 1048575).astype(jnp.int32)
    damping = jnp.clip(jnp.exp(math.log(1.0) - 1.609438 * jax.random.uniform(key_list[1], (NX, NY), jnp.float32) ** shard_levels(key_list[1], (NX, NY), ((0, 8), (1, 4)), -0.2, 0.2)), 0.2, 1.0)
    coupling_x = jnp.clip(jnp.exp(math.log(0.5) - 2.3025851 * jax.random.uniform(key_list[2], (NX, NY), jnp.float32) ** shard_levels(key_list[2], (NX, NY), ((0, 8), (1, 4)), -0.2, 0.2)), 0.05, 0.5)
    coupling_y = jnp.clip(jnp.exp(math.log(0.5) - 2.3025851 * jax.random.uniform(key_list[3], (NX, NY), jnp.float32) ** shard_levels(key_list[3], (NX, NY), ((0, 8), (1, 4)), -0.2, 0.2)), 0.05, 0.5)
    sensor_count = draw_sensor_count(jax.random.fold_in(key_list[7], 71), 0)
    sensor_cells = touch_ends(jax.random.randint(key_list[5], (BX, BY, SMAX), 0, CX * CY), jax.random.fold_in(key_list[5], 1), 0, (CX * CY) - 1).astype(jnp.int32)
    obs_weight = draw_obs_weight(jax.random.fold_in(key_list[7], 71), 0)
    return dict(probe_seeds=probe_seeds, damping=damping, coupling_x=coupling_x, coupling_y=coupling_y, sensor_count=sensor_count, sensor_cells=sensor_cells, obs_weight=obs_weight)


probe_block = 4


def rademacher(seeds, row_ids, col_ids):
    mixed = seeds[:, None, None] * 668265261 + row_ids[None, :, None] * 374761393 + col_ids[None, None, :] * 1103515245
    mixed = (mixed ^ ((mixed >> 16) & 65535)) * 73244475
    mixed = (mixed ^ ((mixed >> 16) & 65535)) * 73244475
    mixed = mixed ^ ((mixed >> 16) & 65535)
    bit_value = (mixed >> 7) & 1
    return (2 * bit_value - 1).astype(jnp.float32)


def apply_operator(field, damping, coupling_x, coupling_y):
    below = jnp.roll(field, -1, 1)
    above = jnp.roll(field, 1, 1)
    right = jnp.roll(field, -1, 2)
    left_side = jnp.roll(field, 1, 2)
    return (damping * field + coupling_x * (field - below) + jnp.roll(coupling_x, 1, 0) * (field - above)
            + coupling_y * (field - right) + jnp.roll(coupling_y, 1, 1) * (field - left_side))


def observe_block(field, count, cell_ids, weight):
    mask = (jnp.arange(SMAX) < count).astype(field.dtype)
    sampled = field[:, cell_ids] * mask
    weighted = jnp.dot(sampled, weight, precision=lax.Precision.HIGHEST) * mask
    return jnp.zeros_like(field).at[:, cell_ids].add(weighted)


def observe(field, sensor_count, sensor_cells, obs_weight):
    group = field.shape[0]
    blocks = field.reshape(group, BX, CX, BY, CY).transpose(1, 3, 0, 2, 4).reshape(BX * BY, group, CX * CY)
    added = jax.vmap(observe_block)(blocks, sensor_count.reshape(-1), sensor_cells.reshape(-1, SMAX),
                                    obs_weight.reshape(-1, SMAX, SMAX))
    return added.reshape(BX, BY, group, CX, CY).transpose(2, 0, 3, 1, 4).reshape(group, NX, NY)


def reference(probe_seeds, damping, coupling_x, coupling_y, sensor_count, sensor_cells, obs_weight):
    row_ids = jnp.arange(NX, dtype=jnp.int32)
    col_ids = jnp.arange(NY, dtype=jnp.int32)

    def hessian(field):
        once = apply_operator(field, damping, coupling_x, coupling_y)
        twice = apply_operator(once, damping, coupling_x, coupling_y)
        return twice + observe(field, sensor_count, sensor_cells, obs_weight)

    def solve_group(seeds):
        probes = rademacher(seeds, row_ids, col_ids)
        norm_start = jnp.sum(probes * probes, axis=(1, 2))
        image = hessian(probes)
        first_step = norm_start / jnp.sum(probes * image, axis=(1, 2))
        solution = first_step[:, None, None] * probes
        residual = probes - first_step[:, None, None] * image
        norm_next = jnp.sum(residual * residual, axis=(1, 2))
        direction = residual + (norm_next / norm_start)[:, None, None] * probes
        image = hessian(direction)
        second_step = norm_next / jnp.sum(direction * image, axis=(1, 2))
        solution = solution + second_step[:, None, None] * direction
        return solution, jnp.sum(probes * solution, axis=(1, 2))

    solutions, products = lax.map(solve_group, probe_seeds.reshape(-1, probe_block))
    return solutions.reshape(PROBES, NX, NY), jnp.sum(products) / PROBES
```

```python
import jax
import jax.numpy as jnp
from jax import lax
from jax.experimental import pallas as pl
from jax.experimental.pallas import tpu as pltpu
from jax.sharding import PartitionSpec as P

LANES = 128
SUBS = 8
F32 = jnp.float32
BF16 = jnp.bfloat16
VMEM = pl.BlockSpec(memory_space=pltpu.VMEM)
SMEM = pl.BlockSpec(memory_space=pltpu.SMEM)


def shifted(value, axis, steps):
    count = lax.axis_size(axis)
    pairs = [(source, (source + steps) % count) for source in range(count)]
    return lax.ppermute(value, axis, pairs)


def sign_bits(seeds, row_ids, col_ids):
    mixed = seeds * 668265261 + row_ids * 374761393 + col_ids * 1103515245
    mixed = (mixed ^ ((mixed >> 16) & 65535)) * 73244475
    mixed = (mixed ^ ((mixed >> 16) & 65535)) * 73244475
    mixed = mixed ^ ((mixed >> 16) & 65535)
    return (2 * ((mixed >> 7) & 1) - 1).astype(F32)


def iota(shape, dim):
    return lax.broadcasted_iota(jnp.int32, shape, dim)


def roll(value, steps, dim):
    return pltpu.roll(value, steps % value.shape[dim], dim)


def pieces(value):
    high = value.astype(BF16)
    rest = value - high.astype(F32)
    middle = rest.astype(BF16)
    low = (rest - middle.astype(F32)).astype(BF16)
    return high, middle, low


def split_cells(cells, block_cols):
    rows = jnp.floor((cells.astype(F32) + 0.5) * (1.0 / block_cols)).astype(jnp.int32)
    return rows, cells - rows * block_cols


def one_hots(cells, block_rows, block_cols):
    rows, cols = split_cells(cells, block_cols)
    slots = cells.shape[1]
    row_hot = jnp.where(iota((block_rows, slots), 0) == rows, 1.0, 0.0)
    col_hot = jnp.where(iota((block_cols, slots), 0) == cols, 1.0, 0.0).astype(BF16)
    return row_hot, col_hot


def side_pack_kernel(d_ref, cx_ref, cy_ref, left_ref, right_ref):
    block_rows, block_cols = d_ref.shape
    lane = iota((block_rows, LANES), 1)
    first = slice(0, LANES)
    last = slice(block_cols - LANES, block_cols)
    left_ref[...] = jnp.where(
        lane < 3,
        cy_ref[:, first],
        jnp.where(lane < 6, roll(d_ref[:, first], 3, 1), roll(cx_ref[:, first], 6, 1)),
    )
    right_ref[...] = jnp.where(
        lane >= LANES - 3,
        cy_ref[:, last],
        jnp.where(lane >= LANES - 6, roll(d_ref[:, last], -3, 1), roll(cx_ref[:, last], -6, 1)),
    )


def side_tiles(from_right, from_left):
    near_right = iota(from_right.shape, 1) < LANES // 2
    cy = jnp.where(near_right, from_right, from_left)
    d = jnp.where(near_right, roll(from_right, -3, 1), roll(from_left, 3, 1))
    cx = jnp.where(near_right, roll(from_right, -6, 1), roll(from_left, 6, 1))
    return d, cx, cy


def observe_kernel(
    seeds_ref, count_ref, cells_ref, weight_ref, probes_ref, obs_ref, left_ref, right_ref
):
    count, wide_rows, wide_cols = probes_ref.shape
    _, block_rows, block_cols = obs_ref.shape
    row_start = lax.axis_index("gx") * block_rows
    col_start = lax.axis_index("gy") * block_cols
    rows_total = lax.axis_size("gx") * block_rows
    cols_total = lax.axis_size("gy") * block_cols

    slots = cells_ref.shape[1]
    cells = cells_ref[...]
    rows, cols = split_cells(cells, block_cols)
    padded = max(SUBS, count)
    which = iota((padded, slots), 0)
    seeds = jnp.zeros((padded, slots), jnp.int32)
    for k in range(count):
        seeds = jnp.where(which == k, seeds_ref[k], seeds)
    live = jnp.where(iota((1, slots), 1) < count_ref[0, 0], 1.0, 0.0)
    sampled = sign_bits(seeds, rows + row_start, cols + col_start) * live
    weighted = (
        jnp.dot(sampled, weight_ref[...], precision=lax.Precision.HIGHEST, preferred_element_type=F32)
        * live
    )
    row_hot, col_hot = one_hots(cells, block_rows, block_cols)
    parts = pieces(weighted)
    stack = [
        (row_hot * part[k : k + 1].astype(F32)).astype(BF16) for k in range(count) for part in parts
    ]
    spread = lax.dot_general(
        jnp.concatenate(stack, 0), col_hot, (((1,), (1,)), ((), ())), preferred_element_type=F32
    )
    lane = iota((block_rows, LANES), 1)
    left = jnp.zeros((block_rows, LANES), F32)
    right = jnp.zeros((block_rows, LANES), F32)
    for k in range(count):
        base = 3 * k * block_rows
        high, middle, low = (
            spread[base + i * block_rows : base + (i + 1) * block_rows] for i in range(3)
        )
        total = (low + middle) + high
        obs_ref[k] = total
        left = jnp.where(lane == k, roll(total[:, :LANES], k, 1), left)
        right = jnp.where(
            lane == LANES - count + k, roll(total[:, block_cols - LANES :], k + 1 - count, 1), right
        )
    left_ref[...] = left
    right_ref[...] = right

    wide = (wide_rows, wide_cols)
    row_ids = iota(wide, 0)
    row_ids = row_start + jnp.where(row_ids >= wide_rows - SUBS, row_ids - wide_rows, row_ids)
    row_ids = jnp.where(row_ids < 0, row_ids + rows_total, row_ids)
    row_ids = jnp.where(row_ids >= rows_total, row_ids - rows_total, row_ids)
    col_ids = iota(wide, 1)
    col_ids = col_start + jnp.where(col_ids >= wide_cols - LANES // 2, col_ids - wide_cols, col_ids)
    col_ids = jnp.where(col_ids < 0, col_ids + cols_total, col_ids)
    col_ids = jnp.where(col_ids >= cols_total, col_ids - cols_total, col_ids)
    for k in range(count):
        probes_ref[k] = sign_bits(seeds_ref[k], row_ids, col_ids)


def edge_pack_kernel(
    d_ref, cx_ref, cy_ref, from_right_ref, from_left_ref, obs_ref, up_ref, down_ref
):
    count, block_rows, block_cols = obs_ref.shape
    wide_cols = block_cols + LANES
    sub = iota((SUBS, wide_cols), 0)
    nothing = jnp.zeros((1, LANES), F32)

    def wide_rows_of(rows):
        sides = side_tiles(from_right_ref[rows], from_left_ref[rows])
        return [
            jnp.concatenate([ref[rows], side], 1)
            for ref, side in zip((d_ref, cx_ref, cy_ref), sides)
        ]

    def observed(row):
        lines = [
            jnp.concatenate([obs_ref[k, row : row + 1], nothing], 1) for k in range(count)
        ]
        spare = -count % SUBS
        return jnp.concatenate(lines + [jnp.zeros((spare, wide_cols), F32)], 0)

    d, cx, cy = wide_rows_of(slice(0, SUBS))
    up_ref[:SUBS] = jnp.where(sub < 2, cx, jnp.where(sub < 4, roll(d, 2, 0), roll(cy, 4, 0)))
    up_ref[SUBS:] = observed(0)
    d, cx, cy = wide_rows_of(slice(block_rows - SUBS, block_rows))
    down_ref[:SUBS] = jnp.where(
        sub >= SUBS - 3, cx, jnp.where(sub >= SUBS - 5, roll(d, -3, 0), roll(cy, -5, 0))
    )
    down_ref[SUBS:] = observed(block_rows - 1)


def stencil(v, coefs):
    centre, cx, cx_before, cy, cy_before = coefs
    return (
        centre[...] * v
        - cx[...] * roll(v, -1, 0)
        - cx_before[...] * roll(v, 1, 0)
        - cy[...] * roll(v, -1, 1)
        - cy_before[...] * roll(v, 1, 1)
    )


def image_kernel(
    count_ref,
    cells_ref,
    weight_ref,
    d_ref,
    cx_ref,
    cy_ref,
    from_right_ref,
    from_left_ref,
    from_below_ref,
    from_above_ref,
    obs_ref,
    obs_right_ref,
    obs_left_ref,
    probes_ref,
    image_ref,
    sums_ref,
    centre,
    cx_wide,
    cx_before,
    cy_wide,
    cy_before,
):
    count, block_rows, block_cols = obs_ref.shape
    own_rows, own_cols = slice(0, block_rows), slice(0, block_cols)
    below, above = slice(block_rows, block_rows + SUBS), slice(block_rows + SUBS, block_rows + 2 * SUBS)
    side = slice(block_cols, block_cols + LANES)
    d_side, cx_side, cy_side = side_tiles(from_right_ref[...], from_left_ref[...])
    low, high = from_below_ref[:SUBS], from_above_ref[:SUBS]
    for target, own, tile, low_steps, high_steps in (
        (centre, d_ref, d_side, -2, 3),
        (cx_wide, cx_ref, cx_side, 0, 0),
        (cy_wide, cy_ref, cy_side, -4, 5),
    ):
        target[own_rows, own_cols] = own[...]
        target[own_rows, side] = tile
        target[below] = roll(low, low_steps, 0) if low_steps else low
        target[above] = roll(high, high_steps, 0) if high_steps else high
    cx, cy = cx_wide[...], cy_wide[...]
    cx_up, cy_left = roll(cx, 1, 0), roll(cy, 1, 1)
    cx_before[...] = cx_up
    cy_before[...] = cy_left
    centre[...] = centre[...] + (cx + cx_up) + (cy + cy_left)
    coefs = (centre, cx_wide, cx_before, cy_wide, cy_before)

    slots = cells_ref.shape[1]
    row_hot, col_hot = one_hots(cells_ref[...], block_rows, block_cols)
    live = jnp.where(iota((1, slots), 1) < count_ref[0, 0], 1.0, 0.0)
    lane = iota((block_rows, LANES), 1)
    sub = iota((SUBS, block_cols + LANES), 0)
    stack, lines = [], []
    for k in range(count):
        probe = probes_ref[k]
        once = stencil(probe, coefs)
        right = jnp.where(lane == 0, roll(obs_right_ref[...], -k, 1), 0.0)
        left = jnp.where(lane == LANES - 1, roll(obs_left_ref[...], count - 1 - k, 1), right)
        under = jnp.where(sub == 0, from_below_ref[SUBS + k : SUBS + k + 1], 0.0)
        over = jnp.where(sub == SUBS - 1, from_above_ref[SUBS + k : SUBS + k + 1], 0.0)
        seen = jnp.concatenate([jnp.concatenate([obs_ref[k], left], 1), under, over], 0)
        image = stencil(once, coefs) + seen
        applied = stencil(image, coefs)[own_rows, own_cols]
        image = image[own_rows, own_cols]
        image_ref[k] = image
        stack.extend(pieces(image))
        lines.append(jnp.sum(probe[own_rows, own_cols] * image, 0, keepdims=True))
        lines.append(jnp.sum(image * image, 0, keepdims=True))
        lines.append(jnp.sum(applied * applied, 0, keepdims=True))
    found = jnp.dot(jnp.concatenate(stack, 0), col_hot, preferred_element_type=F32)
    sampled = []
    for k in range(count):
        base = 3 * k * block_rows
        high, middle, low = (
            found[base + i * block_rows : base + (i + 1) * block_rows] for i in range(3)
        )
        sampled.append(jnp.sum(((low + middle) + high) * row_hot, 0, keepdims=True) * live)
    spare = -count % SUBS
    sampled = jnp.concatenate(sampled + [jnp.zeros((spare, slots), F32)], 0)
    weighted = jnp.dot(
        sampled, weight_ref[...], precision=lax.Precision.HIGHEST, preferred_element_type=F32
    )
    product = jnp.sum(sampled * weighted, 1, keepdims=True)
    total = jnp.zeros((1, LANES), F32)
    out_lane = iota((1, LANES), 1)
    for k in range(count):
        for i in range(3):
            value = jnp.sum(lines[3 * k + i], 1, keepdims=True)
            if i == 2:
                value = value + product[k : k + 1]
            total = jnp.where(out_lane == i * count + k, value, total)
    sums_ref[...] = jnp.broadcast_to(total[None], sums_ref.shape)


def finish_kernel(sums_ref, probes_ref, image_ref, solution_ref, trace_ref):
    count, block_rows, block_cols = image_ref.shape
    cells_total = float(block_rows * block_cols * sums_ref.shape[0])
    first = jnp.sum(sums_ref[...], 0)
    second = roll(first, -count, 1)
    third = roll(first, -2 * count, 1)
    step = cells_total / first
    growth = step * step * second * (1.0 / cells_total)
    ratio = growth - 1.0
    bend = step * step * step * third * (1.0 / cells_total) - growth * growth
    next_step = step * ratio / bend
    on_probe = step + next_step * growth
    on_image = step * next_step
    used = iota(first.shape, 1) < count
    trace = jnp.where(used, step + next_step * ratio, 0.0)
    trace_ref[...] = jnp.sum(trace, 1, keepdims=True) * (cells_total / count)
    for k in range(count):
        solution_ref[k] = (
            on_probe[:, k : k + 1] * probes_ref[k, :block_rows, :block_cols]
            - on_image[:, k : k + 1] * image_ref[k]
        )


def per_device(
    probe_seeds, damping, coupling_x, coupling_y, sensor_count, sensor_cells, obs_weight
):
    block_rows, block_cols = damping.shape
    count = probe_seeds.shape[0]
    slots = obs_weight.shape[-1]
    cells = sensor_cells.reshape(1, slots)
    weight = obs_weight.reshape(slots, slots)
    wide_rows, wide_cols = block_rows + 2 * SUBS, block_cols + LANES
    devices = lax.axis_size("gx") * lax.axis_size("gy")
    full = jax.ShapeDtypeStruct

    to_left, to_right = pl.pallas_call(
        side_pack_kernel,
        out_shape=[full((block_rows, LANES), F32)] * 2,
        in_specs=[VMEM] * 3,
        out_specs=[VMEM] * 2,
    )(damping, coupling_x, coupling_y)
    from_right = shifted(to_left, "gy", -1)
    from_left = shifted(to_right, "gy", 1)

    probes, observed, obs_to_left, obs_to_right = pl.pallas_call(
        observe_kernel,
        out_shape=[
            full((count, wide_rows, wide_cols), F32),
            full((count, block_rows, block_cols), F32),
            full((block_rows, LANES), F32),
            full((block_rows, LANES), F32),
        ],
        in_specs=[SMEM, SMEM, VMEM, VMEM],
        out_specs=[VMEM] * 4,
    )(probe_seeds, sensor_count, cells, weight)

    edge_rows = SUBS + count + -count % SUBS
    to_above, to_below = pl.pallas_call(
        edge_pack_kernel,
        out_shape=[full((edge_rows, wide_cols), F32)] * 2,
        in_specs=[VMEM] * 6,
        out_specs=[VMEM] * 2,
    )(damping, coupling_x, coupling_y, from_right, from_left, observed)
    from_below = shifted(to_above, "gx", -1)
    from_above = shifted(to_below, "gx", 1)
    obs_right = shifted(obs_to_left, "gy", -1)
    obs_left = shifted(obs_to_right, "gy", 1)

    image, sums = pl.pallas_call(
        image_kernel,
        out_shape=[full((count, block_rows, block_cols), F32), full((devices, 1, LANES), F32)],
        in_specs=[SMEM] + [VMEM] * 13,
        out_specs=[VMEM] * 2,
        scratch_shapes=[pltpu.VMEM((wide_rows, wide_cols), F32)] * 5,
    )(
        sensor_count,
        cells,
        weight,
        damping,
        coupling_x,
        coupling_y,
        from_right,
        from_left,
        from_below,
        from_above,
        observed,
        obs_right,
        obs_left,
        probes,
    )
    sums = lax.all_to_all(sums, ("gx", "gy"), 0, 0, tiled=True)
    solved, trace = pl.pallas_call(
        finish_kernel,
        out_shape=[full((count, block_rows, block_cols), F32), full((1, 1), F32)],
        in_specs=[VMEM] * 3,
        out_specs=[VMEM] * 2,
    )(sums, probes, image)
    return solved, trace[0, 0]


def solution(mesh):
    placed = (
        P(),
        P("gx", "gy"),
        P("gx", "gy"),
        P("gx", "gy"),
        P("gx", "gy"),
        P("gx", "gy", None),
        P("gx", "gy", None, None),
    )
    return jax.shard_map(
        per_device,
        mesh=mesh,
        in_specs=placed,
        out_specs=(P(None, "gx", "gy"), P()),
        check_vma=False,
    )
```

```python
import jax
import jax.numpy as jnp
from jax import lax
from jax.experimental import pallas as pl
from jax.experimental.pallas import tpu as pltpu
from jax.sharding import PartitionSpec as P

LANES = 128
SUBS = 8
F32 = jnp.float32
BF16 = jnp.bfloat16
SMEM = pl.BlockSpec(memory_space=pltpu.SMEM)
VMEM = pl.BlockSpec(memory_space=pltpu.VMEM)


def shifted(value, axis, steps):
    count = lax.axis_size(axis)
    pairs = [(source, (source + steps) % count) for source in range(count)]
    return lax.ppermute(value, axis, pairs)


def on_chip(*values):
    return tuple(pltpu.with_memory_space_constraint(value, pltpu.VMEM) for value in values)


def sign_bits(seeds, row_ids, col_ids):
    mixed = seeds * 668265261 + row_ids * 374761393 + col_ids * 1103515245
    mixed = (mixed ^ ((mixed >> 16) & 65535)) * 73244475
    mixed = (mixed ^ ((mixed >> 16) & 65535)) * 73244475
    mixed = mixed ^ ((mixed >> 16) & 65535)
    return (2 * ((mixed >> 7) & 1) - 1).astype(F32)


def iota(shape, dim):
    return lax.broadcasted_iota(jnp.int32, shape, dim)


def roll(value, steps, dim):
    return pltpu.roll(value, steps % value.shape[dim], dim)


def pieces(value):
    high = value.astype(BF16)
    rest = value - high.astype(F32)
    middle = rest.astype(BF16)
    low = (rest - middle.astype(F32)).astype(BF16)
    return high, middle, low


def split_cells(cells, block_cols):
    rows = jnp.floor((cells.astype(F32) + 0.5) * (1.0 / block_cols)).astype(jnp.int32)
    return rows, cells - rows * block_cols


def one_hots(cells, block_rows, block_cols):
    rows, cols = split_cells(cells, block_cols)
    slots = cells.shape[1]
    row_hot = jnp.where(iota((block_rows, slots), 0) == rows, 1.0, 0.0)
    col_hot = jnp.where(iota((block_cols, slots), 0) == cols, 1.0, 0.0).astype(BF16)
    return row_hot, col_hot


def load_kernel(
    seeds_in, cells_in, weight_in, d_in, cx_in, cy_in,
    seeds_ref, cells_ref, weight_ref, d_ref, cx_ref, cy_ref, left_ref, right_ref,
):
    block_rows, block_cols = d_in.shape
    d, cx, cy = d_in[...], cx_in[...], cy_in[...]
    d_ref[...], cx_ref[...], cy_ref[...] = d, cx, cy
    lane = iota((block_rows, LANES), 1)
    left_ref[...] = jnp.where(
        lane < 3,
        cy[:, :LANES],
        jnp.where(lane < 6, roll(d[:, :LANES], 3, 1), roll(cx[:, :LANES], 6, 1)),
    )
    last = slice(block_cols - LANES, block_cols)
    right_ref[...] = jnp.where(
        lane >= LANES - 3,
        cy[:, last],
        jnp.where(lane >= LANES - 6, roll(d[:, last], -3, 1), roll(cx[:, last], -6, 1)),
    )
    seeds_ref[...] = seeds_in[...]
    cells_ref[...] = cells_in[...]
    weight_ref[...] = weight_in[...]


def side_tiles(from_right, from_left):
    near_right = iota(from_right.shape, 1) < LANES // 2
    cy = jnp.where(near_right, from_right, from_left)
    d = jnp.where(near_right, roll(from_right, -3, 1), roll(from_left, 3, 1))
    cx = jnp.where(near_right, roll(from_right, -6, 1), roll(from_left, 6, 1))
    return d, cx, cy


def observe_kernel(
    number_ref, seeds_ref, cells_ref, weight_ref, probes_ref, obs_ref, live_ref
):
    count, wide_rows, wide_cols = probes_ref.shape
    _, block_rows, block_cols = obs_ref.shape
    row_start = lax.axis_index("gx") * block_rows
    col_start = lax.axis_index("gy") * block_cols
    rows_total = lax.axis_size("gx") * block_rows
    cols_total = lax.axis_size("gy") * block_cols

    slots = cells_ref.shape[1]
    cells = cells_ref[...]
    rows, cols = split_cells(cells, block_cols)
    padded = max(SUBS, count)
    which = iota((padded, slots), 0)
    seeds = jnp.zeros((padded, slots), jnp.int32)
    for k in range(count):
        seeds = jnp.where(which == k, seeds_ref[:, k : k + 1], seeds)
    live = jnp.where(iota((1, slots), 1) < number_ref[0, 0], 1.0, 0.0)
    live_ref[...] = live
    sampled = sign_bits(seeds, rows + row_start, cols + col_start) * live
    weighted = (
        jnp.dot(sampled, weight_ref[...], precision=lax.Precision.HIGHEST, preferred_element_type=F32)
        * live
    )
    row_hot, col_hot = one_hots(cells, block_rows, block_cols)
    parts = pieces(weighted)
    stack = [
        (row_hot * part[k : k + 1].astype(F32)).astype(BF16) for k in range(count) for part in parts
    ]
    spread = lax.dot_general(
        jnp.concatenate(stack, 0), col_hot, (((1,), (1,)), ((), ())), preferred_element_type=F32
    )
    for k in range(count):
        base = 3 * k * block_rows
        high, middle, low = (
            spread[base + i * block_rows : base + (i + 1) * block_rows] for i in range(3)
        )
        obs_ref[k] = (low + middle) + high

    wide = (wide_rows, wide_cols)
    row_ids = iota(wide, 0)
    row_ids = row_start + jnp.where(row_ids >= wide_rows - SUBS, row_ids - wide_rows, row_ids)
    row_ids = jnp.where(row_ids < 0, row_ids + rows_total, row_ids)
    row_ids = jnp.where(row_ids >= rows_total, row_ids - rows_total, row_ids)
    col_ids = iota(wide, 1)
    col_ids = col_start + jnp.where(col_ids >= wide_cols - LANES // 2, col_ids - wide_cols, col_ids)
    col_ids = jnp.where(col_ids < 0, col_ids + cols_total, col_ids)
    col_ids = jnp.where(col_ids >= cols_total, col_ids - cols_total, col_ids)
    for k in range(count):
        probes_ref[k] = sign_bits(seeds_ref[:, k : k + 1], row_ids, col_ids)


def edge_pack_kernel(
    d_ref, cx_ref, cy_ref, from_right_ref, from_left_ref, obs_ref,
    up_ref, down_ref, left_ref, right_ref,
):
    count, block_rows, block_cols = obs_ref.shape
    wide_cols = block_cols + LANES
    sub = iota((SUBS, wide_cols), 0)
    nothing = jnp.zeros((1, LANES), F32)

    def wide_rows_of(rows):
        sides = side_tiles(from_right_ref[rows], from_left_ref[rows])
        return [
            jnp.concatenate([ref[rows], side], 1)
            for ref, side in zip((d_ref, cx_ref, cy_ref), sides)
        ]

    def observed(row):
        lines = [
            jnp.concatenate([obs_ref[k, row : row + 1], nothing], 1) for k in range(count)
        ]
        spare = -count % SUBS
        return jnp.concatenate(lines + [jnp.zeros((spare, wide_cols), F32)], 0)

    d, cx, cy = wide_rows_of(slice(0, SUBS))
    up_ref[:SUBS] = jnp.where(sub < 2, cx, jnp.where(sub < 4, roll(d, 2, 0), roll(cy, 4, 0)))
    up_ref[SUBS:] = observed(0)
    d, cx, cy = wide_rows_of(slice(block_rows - SUBS, block_rows))
    down_ref[:SUBS] = jnp.where(
        sub >= SUBS - 3, cx, jnp.where(sub >= SUBS - 5, roll(d, -3, 0), roll(cy, -5, 0))
    )
    down_ref[SUBS:] = observed(block_rows - 1)
    lane = iota((block_rows, LANES), 1)
    left = jnp.zeros((block_rows, LANES), F32)
    right = jnp.zeros((block_rows, LANES), F32)
    for k in range(count):
        left = jnp.where(lane == k, roll(obs_ref[k, :, :LANES], k, 1), left)
        last = obs_ref[k, :, block_cols - LANES :]
        right = jnp.where(lane == LANES - count + k, roll(last, k + 1 - count, 1), right)
    left_ref[...] = left
    right_ref[...] = right


def stencil(v, coefs):
    centre, cx, cx_before, cy, cy_before = coefs
    return (
        centre[...] * v
        - cx[...] * roll(v, -1, 0)
        - cx_before[...] * roll(v, 1, 0)
        - cy[...] * roll(v, -1, 1)
        - cy_before[...] * roll(v, 1, 1)
    )


def image_kernel(
    live_ref,
    cells_ref,
    weight_ref,
    d_ref,
    cx_ref,
    cy_ref,
    from_right_ref,
    from_left_ref,
    from_below_ref,
    from_above_ref,
    obs_ref,
    obs_right_ref,
    obs_left_ref,
    probes_ref,
    image_ref,
    sums_ref,
    centre,
    cx_wide,
    cx_before,
    cy_wide,
    cy_before,
):
    count, block_rows, block_cols = obs_ref.shape
    own_rows, own_cols = slice(0, block_rows), slice(0, block_cols)
    below, above = slice(block_rows, block_rows + SUBS), slice(block_rows + SUBS, block_rows + 2 * SUBS)
    side = slice(block_cols, block_cols + LANES)
    d_side, cx_side, cy_side = side_tiles(from_right_ref[...], from_left_ref[...])
    low, high = from_below_ref[:SUBS], from_above_ref[:SUBS]
    for target, own, tile, low_steps, high_steps in (
        (centre, d_ref, d_side, -2, 3),
        (cx_wide, cx_ref, cx_side, 0, 0),
        (cy_wide, cy_ref, cy_side, -4, 5),
    ):
        target[own_rows, own_cols] = own[...]
        target[own_rows, side] = tile
        target[below] = roll(low, low_steps, 0) if low_steps else low
        target[above] = roll(high, high_steps, 0) if high_steps else high
    cx, cy = cx_wide[...], cy_wide[...]
    cx_up, cy_left = roll(cx, 1, 0), roll(cy, 1, 1)
    cx_before[...] = cx_up
    cy_before[...] = cy_left
    centre[...] = centre[...] + (cx + cx_up) + (cy + cy_left)
    coefs = (centre, cx_wide, cx_before, cy_wide, cy_before)

    slots = cells_ref.shape[1]
    row_hot, col_hot = one_hots(cells_ref[...], block_rows, block_cols)
    live = live_ref[...]
    lane = iota((block_rows, LANES), 1)
    sub = iota((SUBS, block_cols + LANES), 0)
    stack, lines = [], []
    for k in range(count):
        probe = probes_ref[k]
        once = stencil(probe, coefs)
        right = jnp.where(lane == 0, roll(obs_right_ref[...], -k, 1), 0.0)
        left = jnp.where(lane == LANES - 1, roll(obs_left_ref[...], count - 1 - k, 1), right)
        under = jnp.where(sub == 0, from_below_ref[SUBS + k : SUBS + k + 1], 0.0)
        over = jnp.where(sub == SUBS - 1, from_above_ref[SUBS + k : SUBS + k + 1], 0.0)
        seen = jnp.concatenate([jnp.concatenate([obs_ref[k], left], 1), under, over], 0)
        image = stencil(once, coefs) + seen
        applied = stencil(image, coefs)[own_rows, own_cols]
        image = image[own_rows, own_cols]
        image_ref[k] = image
        stack.extend(pieces(image))
        lines.append(jnp.sum(probe[own_rows, own_cols] * image, 0, keepdims=True))
        lines.append(jnp.sum(image * image, 0, keepdims=True))
        lines.append(jnp.sum(applied * applied, 0, keepdims=True))
    found = jnp.dot(jnp.concatenate(stack, 0), col_hot, preferred_element_type=F32)
    sampled = []
    for k in range(count):
        base = 3 * k * block_rows
        high, middle, low = (
            found[base + i * block_rows : base + (i + 1) * block_rows] for i in range(3)
        )
        sampled.append(jnp.sum(((low + middle) + high) * row_hot, 0, keepdims=True) * live)
    spare = -count % SUBS
    sampled = jnp.concatenate(sampled + [jnp.zeros((spare, slots), F32)], 0)
    weighted = jnp.dot(
        sampled, weight_ref[...], precision=lax.Precision.HIGHEST, preferred_element_type=F32
    )
    product = jnp.sum(sampled * weighted, 1, keepdims=True)
    total = jnp.zeros((1, LANES), F32)
    out_lane = iota((1, LANES), 1)
    for k in range(count):
        for i in range(3):
            value = jnp.sum(lines[3 * k + i], 1, keepdims=True)
            if i == 2:
                value = value + product[k : k + 1]
            total = jnp.where(out_lane == i * count + k, value, total)
    sums_ref[...] = jnp.broadcast_to(total[None], sums_ref.shape)


def finish_kernel(sums_ref, probes_ref, image_ref, solution_ref, trace_ref):
    count, block_rows, block_cols = image_ref.shape
    cells_total = float(block_rows * block_cols * sums_ref.shape[0])
    first = jnp.sum(sums_ref[...], 0)
    second = roll(first, -count, 1)
    third = roll(first, -2 * count, 1)
    step = cells_total / first
    growth = step * step * second * (1.0 / cells_total)
    ratio = growth - 1.0
    bend = step * step * step * third * (1.0 / cells_total) - growth * growth
    next_step = step * ratio / bend
    on_probe = step + next_step * growth
    on_image = step * next_step
    used = iota(first.shape, 1) < count
    trace = jnp.where(used, step + next_step * ratio, 0.0)
    trace_ref[...] = jnp.sum(trace, 1, keepdims=True) * (cells_total / count)
    for k in range(count):
        solution_ref[k] = (
            on_probe[:, k : k + 1] * probes_ref[k, :block_rows, :block_cols]
            - on_image[:, k : k + 1] * image_ref[k]
        )


def per_device(
    probe_seeds, damping, coupling_x, coupling_y, sensor_count, sensor_cells, obs_weight
):
    block_rows, block_cols = damping.shape
    count = probe_seeds.shape[0]
    slots = obs_weight.shape[-1]
    wide_rows, wide_cols = block_rows + 2 * SUBS, block_cols + LANES
    devices = lax.axis_size("gx") * lax.axis_size("gy")
    edge_rows = SUBS + count + -count % SUBS
    full = jax.ShapeDtypeStruct

    def call(kernel, args, outs, scratch=(), scalars=0):
        return pl.pallas_call(
            kernel,
            out_shape=outs,
            in_specs=[SMEM] * scalars + [VMEM] * (len(args) - scalars),
            out_specs=[VMEM] * len(outs),
            scratch_shapes=scratch,
        )(*args)

    block = pltpu.VMEM((block_rows, block_cols), F32)
    blocks = pltpu.VMEM((count, block_rows, block_cols), F32)
    wide_blocks = pltpu.VMEM((count, wide_rows, wide_cols), F32)
    column = pltpu.VMEM((block_rows, LANES), F32)
    rows = pltpu.VMEM((edge_rows, wide_cols), F32)

    seeds, cells, weight, *coefs, to_left, to_right = call(
        load_kernel,
        (
            probe_seeds.reshape(1, count),
            sensor_cells.reshape(1, slots),
            obs_weight.reshape(slots, slots),
            damping,
            coupling_x,
            coupling_y,
        ),
        [
            pltpu.VMEM((1, count), jnp.int32),
            pltpu.VMEM((1, slots), jnp.int32),
            pltpu.VMEM((slots, slots), F32),
            block,
            block,
            block,
            column,
            column,
        ],
    )
    seeds, cells, weight, *coefs = on_chip(seeds, cells, weight, *coefs)
    from_right = shifted(to_left, "gy", -1)
    from_left = shifted(to_right, "gy", 1)
    sides = on_chip(from_right, from_left)

    probes, observed, live = on_chip(
        *call(
            observe_kernel,
            (sensor_count, seeds, cells, weight),
            [wide_blocks, blocks, pltpu.VMEM((1, slots), F32)],
            scalars=1,
        )
    )
    to_above, to_below, obs_to_left, obs_to_right = call(
        edge_pack_kernel, (*coefs, *sides, observed), [rows, rows, column, column]
    )
    from_below = shifted(to_above, "gx", -1)
    from_above = shifted(to_below, "gx", 1)
    obs_right = shifted(obs_to_left, "gy", -1)
    obs_left = shifted(obs_to_right, "gy", 1)

    image, sums = call(
        image_kernel,
        (
            live,
            cells,
            weight,
            *coefs,
            *sides,
            *on_chip(from_below, from_above),
            observed,
            *on_chip(obs_right, obs_left),
            probes,
        ),
        [blocks, pltpu.VMEM((devices, 1, LANES), F32)],
        [pltpu.VMEM((wide_rows, wide_cols), F32)] * 5,
    )
    sums = lax.all_to_all(sums, ("gx", "gy"), 0, 0, tiled=True)
    solved, trace = call(
        finish_kernel,
        (*on_chip(sums), probes, *on_chip(image)),
        [full((count, block_rows, block_cols), F32), full((1, 1), F32)],
    )
    return solved, trace[0, 0]


def solution(mesh):
    placed = (
        P(),
        P("gx", "gy"),
        P("gx", "gy"),
        P("gx", "gy"),
        P("gx", "gy"),
        P("gx", "gy", None),
        P("gx", "gy", None, None),
    )
    return jax.shard_map(
        per_device,
        mesh=mesh,
        in_specs=placed,
        out_specs=(P(None, "gx", "gy"), P()),
        check_vma=False,
    )
```

```python
import jax
import jax.numpy as jnp
from jax import lax
from jax.experimental import pallas as pl
from jax.experimental.pallas import tpu as pltpu
from jax.sharding import PartitionSpec as P


LANES = 128
SUBS = 8
F32 = jnp.float32
BF16 = jnp.bfloat16
SMEM = pl.BlockSpec(memory_space=pltpu.SMEM)
VMEM = pl.BlockSpec(memory_space=pltpu.VMEM)


def shifted(value, axis, steps):
    count = lax.axis_size(axis)
    pairs = [(source, (source + steps) % count) for source in range(count)]
    return lax.ppermute(value, axis, pairs)


def shifted_both(value):
    down, across = lax.axis_size("gx"), lax.axis_size("gy")
    pairs = [
        (x * across + y, (x + 1) % down * across + (y + 1) % across)
        for x in range(down)
        for y in range(across)
    ]
    return lax.ppermute(value, ("gx", "gy"), pairs)


def on_chip(*values):
    return tuple(pltpu.with_memory_space_constraint(value, pltpu.VMEM) for value in values)


def sign_bits(seeds, row_ids, col_ids):
    mixed = seeds * 668265261 + row_ids * 374761393 + col_ids * 1103515245
    mixed = (mixed ^ ((mixed >> 16) & 65535)) * 73244475
    mixed = (mixed ^ ((mixed >> 16) & 65535)) * 73244475
    mixed = mixed ^ ((mixed >> 16) & 65535)
    return (2 * ((mixed >> 7) & 1) - 1).astype(F32)


def iota(shape, dim):
    return lax.broadcasted_iota(jnp.int32, shape, dim)


def roll(value, steps, dim):
    return pltpu.roll(value, steps % value.shape[dim], dim)


def pieces(value):
    high = value.astype(BF16)
    rest = value - high.astype(F32)
    middle = rest.astype(BF16)
    low = (rest - middle.astype(F32)).astype(BF16)
    return high, middle, low


def split_cells(cells, block_cols):
    rows = jnp.floor((cells.astype(F32) + 0.5) * (1.0 / block_cols)).astype(jnp.int32)
    return rows, cells - rows * block_cols


def one_hots(cells, block_rows, block_cols):
    rows, cols = split_cells(cells, block_cols)
    slots = cells.shape[1]
    row_hot = jnp.where(iota((block_rows, slots), 0) == rows, 1.0, 0.0)
    col_hot = jnp.where(iota((block_cols, slots), 0) == cols, 1.0, 0.0).astype(BF16)
    return row_hot, col_hot


def compact(value, width):
    per = LANES // width
    tiles = value.shape[0] // SUBS
    lane = iota((SUBS, LANES), 1)
    packed = []
    for start in range(0, tiles, per):
        total = value[start * SUBS : (start + 1) * SUBS]
        for i in range(1, min(per, tiles - start)):
            tile = value[(start + i) * SUBS : (start + i + 1) * SUBS]
            total = jnp.where(lane < LANES - width * i, roll(tile, -width * i, 1), total)
        packed.append(total)
    return packed[0] if len(packed) == 1 else jnp.concatenate(packed, 0)


def expand(packed, rows, width):
    per = LANES // width
    tiles = []
    for i in range(rows // SUBS):
        start = i // per * SUBS
        tile = packed[start : start + SUBS]
        tiles.append(roll(tile, width * (i % per), 1) if i % per else tile)
    return jnp.concatenate(tiles, 0)


def compact_rows(rows, width):
    per = LANES // width
    return SUBS * (-(-rows // SUBS // per))


def side_width(count):
    width = 1
    while width < 13 + 3 * count:
        width *= 2
    return width


BACK_WIDTH = 8
HALO = 5


def start_kernel(
    number_ref, seeds_ref, cells_in, weight_in, d_in, cx_in, cy_in,
    cells_ref, weight_ref, d_ref, cx_ref, cy_ref, obs_ref, live_ref,
    rows_next_ref, cols_next_ref, diag_next_ref, rows_back_ref, cols_back_ref,
):
    count, block_rows, block_cols = obs_ref.shape
    row_start = lax.axis_index("gx") * block_rows
    col_start = lax.axis_index("gy") * block_cols
    slots = cells_in.shape[1]
    cells = cells_in[...]
    weight = weight_in[...]
    cells_ref[...] = cells
    weight_ref[...] = weight
    rows, cols = split_cells(cells, block_cols)
    padded = count + -count % SUBS
    which = iota((padded, slots), 0)
    seeds = jnp.zeros((padded, slots), jnp.int32)
    for k in range(count):
        seeds = jnp.where(which == k, seeds_ref[:, k : k + 1], seeds)
    live = jnp.where(iota((1, slots), 1) < number_ref[0, 0], 1.0, 0.0)
    live_ref[...] = live
    sampled = sign_bits(seeds, rows + row_start, cols + col_start) * live
    weighted = (
        jnp.dot(sampled, weight, precision=lax.Precision.HIGHEST, preferred_element_type=F32) * live
    )
    row_hot, col_hot = one_hots(cells, block_rows, block_cols)
    parts = pieces(weighted)
    stack = [
        (row_hot * part[k : k + 1].astype(F32)).astype(BF16) for k in range(count) for part in parts
    ]
    spread = lax.dot_general(
        jnp.concatenate(stack, 0), col_hot, (((1,), (1,)), ((), ())), preferred_element_type=F32
    )
    observed = []
    for k in range(count):
        base = 3 * k * block_rows
        high, middle, low = (
            spread[base + i * block_rows : base + (i + 1) * block_rows] for i in range(3)
        )
        observed.append((low + middle) + high)
        obs_ref[k] = observed[k]

    d, cx, cy = d_in[...], cx_in[...], cy_in[...]
    d_ref[...], cx_ref[...], cy_ref[...] = d, cx, cy
    tail = slice(block_rows - SUBS, block_rows)
    last = slice(block_cols - LANES, block_cols)

    sub = iota((SUBS, block_cols), 0)
    rows_next_ref[:SUBS] = cx[tail]
    rows_next_ref[SUBS : 2 * SUBS] = jnp.where(sub >= 4, d[tail], roll(cy[tail], -4, 0))
    for k in range(0, count, 2):
        tile = observed[k][tail]
        if k + 1 < count:
            tile = jnp.where(sub >= 5, tile, roll(observed[k + 1][tail], -3, 0))
        rows_next_ref[(2 + k // 2) * SUBS : (3 + k // 2) * SUBS] = tile

    lane = iota((block_rows, LANES), 1)
    side = jnp.where(lane >= LANES - 5, cy[:, last], roll(d[:, last], -5, 1))
    side = jnp.where(lane >= LANES - 9, side, roll(cx[:, last], -9, 1))
    for k in range(count):
        edge = LANES - 13 - 3 * k
        side = jnp.where(lane >= edge, side, roll(observed[k][:, last], edge, 1))
    cols_next_ref[...] = compact(side, side_width(count))

    lane = iota((SUBS, LANES), 1)
    corner = d[tail, last]
    for i, value in enumerate([cx, cy] + observed):
        edge = LANES - HALO * (i + 1)
        corner = jnp.where(lane >= edge, corner, roll(value[tail, last], edge, 1))
    diag_next_ref[...] = corner

    rows_back_ref[...] = jnp.where(
        sub == 0, cx[:SUBS], jnp.where(sub == 1, roll(d[:SUBS], 1, 0), roll(cy[:SUBS], 2, 0))
    )
    lane = iota((block_rows, LANES), 1)
    back = jnp.where(lane == LANES - 1, roll(cy[:, :LANES], -1, 1), roll(d[:, :LANES], -2, 1))
    back = jnp.where(lane >= LANES - 2, back, roll(cx[:, :LANES], -3, 1))
    cols_back_ref[...] = compact(back, BACK_WIDTH)


def probes_kernel(seeds_ref, probes_ref):
    count, wide_rows, wide_cols = probes_ref.shape
    block_rows, block_cols = wide_rows - 2 * SUBS, wide_cols - LANES
    row_start = lax.axis_index("gx") * block_rows
    col_start = lax.axis_index("gy") * block_cols
    rows_total = lax.axis_size("gx") * block_rows
    cols_total = lax.axis_size("gy") * block_cols
    wide = (wide_rows, wide_cols)
    row_ids = iota(wide, 0)
    row_ids = row_start + jnp.where(row_ids >= wide_rows - SUBS, row_ids - wide_rows, row_ids)
    row_ids = jnp.where(row_ids < 0, row_ids + rows_total, row_ids)
    row_ids = jnp.where(row_ids >= rows_total, row_ids - rows_total, row_ids)
    col_ids = iota(wide, 1)
    col_ids = col_start + jnp.where(col_ids >= wide_cols - LANES // 2, col_ids - wide_cols, col_ids)
    col_ids = jnp.where(col_ids < 0, col_ids + cols_total, col_ids)
    col_ids = jnp.where(col_ids >= cols_total, col_ids - cols_total, col_ids)
    for k in range(count):
        probes_ref[k] = sign_bits(seeds_ref[:, k : k + 1], row_ids, col_ids)


def stencil(v, coefs):
    centre, cx, cx_before, cy, cy_before = coefs
    return (
        centre[...] * v
        - cx[...] * roll(v, -1, 0)
        - cx_before[...] * roll(v, 1, 0)
        - cy[...] * roll(v, -1, 1)
        - cy_before[...] * roll(v, 1, 1)
    )


def image_kernel(
    live_ref, cells_ref, weight_ref, d_ref, cx_ref, cy_ref, obs_ref,
    above_ref, left_ref, corner_ref, below_ref, right_ref, probes_ref,
    image_ref, sums_ref, fix_ref,
    centre, cx_wide, cx_before, cy_wide, cy_before,
):
    count, block_rows, block_cols = obs_ref.shape
    wide_rows, wide_cols = centre.shape
    own = slice(0, block_rows), slice(0, block_cols)
    under, over = slice(block_rows, block_rows + SUBS), slice(block_rows + SUBS, wide_rows)
    main, side = slice(0, block_cols), slice(block_cols, wide_cols)
    left = expand(left_ref[...], block_rows, side_width(count))
    right = expand(right_ref[...], block_rows, BACK_WIDTH)
    corner = corner_ref[...]
    above = above_ref[SUBS : 2 * SUBS]
    below = below_ref[...]
    lane = iota((block_rows, LANES), 1)
    tile_lane = iota((SUBS, LANES), 1)
    nothing = jnp.zeros((SUBS, LANES), F32)
    for target, block, top, bottom, left_steps, right_steps, corner_steps in (
        (centre, d_ref, above, roll(below, -1, 0), 5, 2, 0),
        (cx_wide, cx_ref, above_ref[:SUBS], below, 9, 3, HALO),
        (cy_wide, cy_ref, roll(above, 4, 0), roll(below, -2, 0), 0, 1, 2 * HALO),
    ):
        target[own] = block[...]
        target[over, main] = top
        target[under, main] = bottom
        near = roll(left, left_steps, 1) if left_steps else left
        near = jnp.where(lane >= LANES - HALO, near, 0.0)
        target[own[0], side] = jnp.where(lane == 0, roll(right, right_steps, 1), near)
        tile = roll(corner, corner_steps, 1) if corner_steps else corner
        target[over, side] = jnp.where(tile_lane >= LANES - HALO, tile, 0.0)
        target[under, side] = nothing
    cx, cy = cx_wide[...], cy_wide[...]
    cx_up, cy_left = roll(cx, 1, 0), roll(cy, 1, 1)
    cx_before[...] = cx_up
    cy_before[...] = cy_left
    centre[...] = centre[...] + (cx + cx_up) + (cy + cy_left)
    coefs = (centre, cx_wide, cx_before, cy_wide, cy_before)

    slots = cells_ref.shape[1]
    cells = cells_ref[...]
    row_hot, col_hot = one_hots(cells, block_rows, block_cols)
    live = live_ref[...]
    sub = iota((SUBS, block_cols), 0)
    tile_sub = iota((SUBS, LANES), 0)
    wide_sub = iota((SUBS, wide_cols), 0)
    wide_lane = iota((1, wide_cols), 1)
    kept = jnp.where((wide_lane < block_cols - 2) | (wide_lane >= wide_cols - 2), 1.0, 0.0)

    def summed(value):
        line = jnp.sum(value[: block_rows - SUBS], 0, keepdims=True)
        edge = jnp.where(wide_sub < SUBS - 2, value[block_rows - SUBS : block_rows], value[over])
        return (line + jnp.sum(edge, 0, keepdims=True)) * kept

    stack, lines, first_miss, second_miss = [], [], [], []
    for k in range(count):
        probe = probes_ref[k]
        once = stencil(probe, coefs)
        near = jnp.where(lane >= LANES - 3, roll(left, 13 + 3 * k, 1), 0.0)
        tile = above_ref[(2 + k // 2) * SUBS : (3 + k // 2) * SUBS]
        tile = jnp.where(sub >= SUBS - 3, roll(tile, 3, 0) if k % 2 else tile, 0.0)
        seen_corner = roll(corner, HALO * (3 + k), 1)
        seen_corner = jnp.where((tile_lane >= LANES - 3) & (tile_sub >= SUBS - 3), seen_corner, 0.0)
        seen = jnp.concatenate(
            [
                jnp.concatenate([obs_ref[k], near], 1),
                jnp.zeros((SUBS, wide_cols), F32),
                jnp.concatenate([tile, seen_corner], 1),
            ],
            0,
        )
        image = stencil(once, coefs) + seen
        applied = stencil(image, coefs)
        lines.append([summed(probe * image), summed(image * image), summed(applied * applied)])
        image = image[own]
        image_ref[k] = image
        stack.extend(pieces(image))
        low = block_rows
        first_miss.append(
            cx_ref[low - 1 : low, 0:1]
            * (probe[low : low + 1, wide_cols - 1 : wide_cols] - probe[low : low + 1, 0:1])
        )
        far = slice(block_cols, block_cols + 1)
        second_miss.append(
            cy_ref[0:1, block_cols - 1 : block_cols]
            * (probe[wide_rows - 1 : wide_rows, far] - probe[0:1, far])
        )
    found = jnp.dot(jnp.concatenate(stack, 0), col_hot, preferred_element_type=F32)
    sampled = []
    for k in range(count):
        base = 3 * k * block_rows
        high, middle, low = (
            found[base + i * block_rows : base + (i + 1) * block_rows] for i in range(3)
        )
        sampled.append(jnp.sum(((low + middle) + high) * row_hot, 0, keepdims=True) * live)
    first_hot = jnp.where(cells == (block_rows - 1) * block_cols, live, 0.0)
    second_hot = jnp.where(cells == block_cols - 1, live, 0.0)
    spare = -(count + 2) % SUBS
    points = sampled + [first_hot, second_hot] + [jnp.zeros((spare, slots), F32)] * (spare > 0)
    points = jnp.concatenate(points, 0)
    weighted = jnp.dot(
        points, weight_ref[...], precision=lax.Precision.HIGHEST, preferred_element_type=F32
    )

    def total(value):
        return jnp.sum(value, 1, keepdims=True)

    with_points = total(points * weighted)
    with_first = total(points * weighted[count : count + 1] + weighted * first_hot)
    with_second = total(points * weighted[count + 1 : count + 2] + weighted * second_hot)
    out_lane = iota((1, LANES), 1)
    row = jnp.zeros((1, LANES), F32)
    fix = jnp.zeros((1, LANES), F32)
    for k in range(count):
        one, two = first_miss[k], second_miss[k]
        values = [total(line) for line in lines[k]]
        values[2] = values[2] + with_points[k : k + 1]
        values.append(one * with_first[k : k + 1])
        values.append(two * with_second[k : k + 1])
        values.append(one * one * with_points[count : count + 1])
        values.append(two * two * with_points[count + 1 : count + 2])
        values.append(one * two * with_first[count + 1 : count + 2])
        for i, value in enumerate(values):
            row = jnp.where(out_lane == i * count + k, value, row)
        fix = jnp.where(out_lane == k, one, jnp.where(out_lane == count + k, two, fix))
    row = jnp.where(out_lane == 8 * count, cy_ref[0:1, block_cols - 1 : block_cols], row)
    row = jnp.where(out_lane == 8 * count + 1, cx_ref[block_rows - 1 : block_rows, 0:1], row)
    sums_ref[...] = jnp.broadcast_to(row[None], sums_ref.shape)
    fix_ref[...] = fix


def finish_kernel(sums_ref, probes_ref, image_ref, fix_ref, solution_ref, trace_ref):
    count, block_rows, block_cols = image_ref.shape
    across = lax.axis_size("gy")
    devices = sums_ref.shape[0]
    rows = jnp.sum(sums_ref[...], 1)
    member = iota((devices, 1), 0)
    place = lax.rem(member, across)
    lower = roll(rows, -across, 0)
    lower = jnp.where(place == 0, roll(lower, 1 - across, 0), roll(lower, 1, 0))
    upper = roll(rows, across, 0)
    upper = jnp.where(place == across - 1, roll(upper, across - 1, 0), roll(upper, -1, 0))
    one = lower[:, 8 * count : 8 * count + 1]
    two = upper[:, 8 * count + 1 : 8 * count + 2]
    part = [roll(rows, -i * count, 1) if i else rows for i in range(8)]
    third = part[2] + one * (part[3] + one * part[5] + two * part[7]) + two * (part[4] + two * part[6])

    cells_total = float(block_rows * block_cols * devices)
    first = jnp.sum(part[0], 0, keepdims=True)
    second = jnp.sum(part[1], 0, keepdims=True)
    third = jnp.sum(third, 0, keepdims=True)
    step = cells_total / first
    growth = step * step * second * (1.0 / cells_total)
    ratio = growth - 1.0
    bend = step * step * step * third * (1.0 / cells_total) - growth * growth
    next_step = step * ratio / bend
    on_probe = step + next_step * growth
    on_image = step * next_step
    used = iota(first.shape, 1) < count
    trace = jnp.where(used, step + next_step * ratio, 0.0)
    trace_ref[...] = jnp.sum(trace, 1, keepdims=True) * (cells_total / count)

    mine = member == lax.axis_index("gx") * across + lax.axis_index("gy")
    fix = fix_ref[...]
    change = on_image * fix * jnp.sum(jnp.where(mine, one, 0.0), 0, keepdims=True)
    other = on_image * roll(fix, -count, 1) * jnp.sum(jnp.where(mine, two, 0.0), 0, keepdims=True)
    tile_sub, tile_lane = iota((SUBS, LANES), 0), iota((SUBS, LANES), 1)
    low_left = (tile_sub == SUBS - 1) & (tile_lane == 0)
    high_right = (tile_sub == 0) & (tile_lane == LANES - 1)
    tail = slice(block_rows - SUBS, block_rows)
    last = slice(block_cols - LANES, block_cols)
    for k in range(count):
        here = slice(k, k + 1)
        value = (
            on_probe[:, here] * probes_ref[k, :block_rows, :block_cols]
            - on_image[:, here] * image_ref[k]
        )
        solution_ref[k] = value
        solution_ref[k, tail, :LANES] = solution_ref[k, tail, :LANES] - jnp.where(
            low_left, change[:, here], 0.0
        )
        solution_ref[k, :SUBS, last] = solution_ref[k, :SUBS, last] - jnp.where(
            high_right, other[:, here], 0.0
        )


def per_device(
    probe_seeds, damping, coupling_x, coupling_y, sensor_count, sensor_cells, obs_weight
):
    block_rows, block_cols = damping.shape
    count = probe_seeds.shape[0]
    slots = obs_weight.shape[-1]
    wide_rows, wide_cols = block_rows + 2 * SUBS, block_cols + LANES
    devices = lax.axis_size("gx") * lax.axis_size("gy")
    full = jax.ShapeDtypeStruct

    def call(kernel, args, outs, scratch=(), scalars=0):
        return pl.pallas_call(
            kernel,
            out_shape=outs,
            in_specs=[SMEM] * scalars + [VMEM] * (len(args) - scalars),
            out_specs=[VMEM] * len(outs),
            scratch_shapes=scratch,
        )(*args)

    def space(*shape):
        return pltpu.VMEM(shape, F32)

    block = space(block_rows, block_cols)
    blocks = space(count, block_rows, block_cols)
    seeds = probe_seeds.reshape(1, count)
    outs = call(
        start_kernel,
        (
            sensor_count,
            seeds,
            sensor_cells.reshape(1, slots),
            obs_weight.reshape(slots, slots),
            damping,
            coupling_x,
            coupling_y,
        ),
        [
            pltpu.VMEM((1, slots), jnp.int32),
            space(slots, slots),
            block,
            block,
            block,
            blocks,
            space(1, slots),
            space(SUBS * (2 + (count + 1) // 2), block_cols),
            space(compact_rows(block_rows, side_width(count)), LANES),
            space(SUBS, LANES),
            space(SUBS, block_cols),
            space(compact_rows(block_rows, BACK_WIDTH), LANES),
        ],
        scalars=1,
    )
    cells, weight, *coefs, observed, live = on_chip(*outs[:7])
    rows_next, cols_next, diag_next, rows_back, cols_back = outs[7:]
    above = shifted(rows_next, "gx", 1)
    corner = shifted_both(diag_next)
    left = shifted(cols_next, "gy", 1)
    below = shifted(rows_back, "gx", -1)
    right = shifted(cols_back, "gy", -1)

    probes, = on_chip(
        *call(probes_kernel, (seeds,), [space(count, wide_rows, wide_cols)])
    )
    image, sums, fix = call(
        image_kernel,
        (
            live,
            cells,
            weight,
            *coefs,
            observed,
            *on_chip(above, left, corner, below, right),
            probes,
        ),
        [blocks, space(devices, 1, LANES), space(1, LANES)],
        [space(wide_rows, wide_cols)] * 5,
    )
    sums = lax.all_to_all(sums, ("gx", "gy"), 0, 0, tiled=True)
    solved, trace = call(
        finish_kernel,
        (*on_chip(sums), probes, *on_chip(image, fix)),
        [full((count, block_rows, block_cols), F32), full((1, 1), F32)],
    )
    return solved, trace[0, 0]


def solution(mesh):
    placed = (
        P(),
        P("gx", "gy"),
        P("gx", "gy"),
        P("gx", "gy"),
        P("gx", "gy"),
        P("gx", "gy", None),
        P("gx", "gy", None, None),
    )

    return jax.shard_map(
        per_device,
        mesh=mesh,
        in_specs=placed,
        out_specs=(P(None, "gx", "gy"), P()),
        check_vma=False,
    )
```

```python
import jax
import jax.numpy as jnp
from jax import lax
from jax.experimental import pallas as pl
from jax.experimental.pallas import tpu as pltpu
from jax.sharding import PartitionSpec as P


LANES = 128
SUBS = 8
F32 = jnp.float32
BF16 = jnp.bfloat16
SMEM = pl.BlockSpec(memory_space=pltpu.SMEM)
VMEM = pl.BlockSpec(memory_space=pltpu.VMEM)


def shifted(value, axis, steps):
    count = lax.axis_size(axis)
    pairs = [(source, (source + steps) % count) for source in range(count)]
    return lax.ppermute(value, axis, pairs)


def shifted_both(value):
    down, across = lax.axis_size("gx"), lax.axis_size("gy")
    pairs = [
        (x * across + y, (x + 1) % down * across + (y + 1) % across)
        for x in range(down)
        for y in range(across)
    ]
    return lax.ppermute(value, ("gx", "gy"), pairs)


def on_chip(*values):
    return tuple(pltpu.with_memory_space_constraint(value, pltpu.VMEM) for value in values)


def sign_bits(seeds, row_ids, col_ids):
    mixed = seeds * 668265261 + row_ids * 374761393 + col_ids * 1103515245
    mixed = (mixed ^ ((mixed >> 16) & 65535)) * 73244475
    mixed = (mixed ^ ((mixed >> 16) & 65535)) * 73244475
    mixed = mixed ^ ((mixed >> 16) & 65535)
    return (2 * ((mixed >> 7) & 1) - 1).astype(F32)


def iota(shape, dim):
    return lax.broadcasted_iota(jnp.int32, shape, dim)


def roll(value, steps, dim):
    return pltpu.roll(value, steps % value.shape[dim], dim)


def pieces(value):
    high = value.astype(BF16)
    return high, (value - high.astype(F32)).astype(BF16)


def dot(left, right):
    return jnp.dot(left, right, preferred_element_type=F32)


def split_cells(cells, block_cols):
    rows = jnp.floor((cells.astype(F32) + 0.5) * (1.0 / block_cols)).astype(jnp.int32)
    return rows, cells - rows * block_cols


def one_hots(cells, block_rows, block_cols):
    rows, cols = split_cells(cells, block_cols)
    slots = cells.shape[1]
    row_hot = jnp.where(iota((block_rows, slots), 0) == rows, 1.0, 0.0)
    col_hot = jnp.where(iota((block_cols, slots), 0) == cols, 1.0, 0.0).astype(BF16)
    return row_hot, col_hot


def compact(value, width):
    per = LANES // width
    tiles = value.shape[0] // SUBS
    lane = iota((SUBS, LANES), 1)
    packed = []
    for start in range(0, tiles, per):
        total = value[start * SUBS : (start + 1) * SUBS]
        for i in range(1, min(per, tiles - start)):
            tile = value[(start + i) * SUBS : (start + i + 1) * SUBS]
            total = jnp.where(lane < LANES - width * i, roll(tile, -width * i, 1), total)
        packed.append(total)
    return packed[0] if len(packed) == 1 else jnp.concatenate(packed, 0)


def expand(packed, rows, width):
    per = LANES // width
    tiles = []
    for i in range(rows // SUBS):
        start = i // per * SUBS
        tile = packed[start : start + SUBS]
        tiles.append(roll(tile, width * (i % per), 1) if i % per else tile)
    return jnp.concatenate(tiles, 0)


def compact_rows(rows, width):
    per = LANES // width
    return SUBS * (-(-rows // SUBS // per))


def side_width(count):
    width = 1
    while width < 13 + 3 * count:
        width *= 2
    return width


BACK_WIDTH = 8
HALO = 5


def start_kernel(
    number_ref, seeds_ref, cells_in, weight_in, d_in, cx_in, cy_in,
    seeds_out, cells_ref, high_ref, low_ref, d_ref, cx_ref, cy_ref, obs_ref, live_ref,
    rows_next_ref, cols_next_ref, diag_next_ref, rows_back_ref, cols_back_ref,
):
    count, block_rows, block_cols = obs_ref.shape
    row_start = lax.axis_index("gx") * block_rows
    col_start = lax.axis_index("gy") * block_cols
    slots = cells_in.shape[1]
    cells = cells_in[...]
    seeds_out[...] = seeds_ref[...]
    cells_ref[...] = cells
    weight_high, weight_low = pieces(weight_in[...])
    high_ref[...], low_ref[...] = weight_high, weight_low
    rows, cols = split_cells(cells, block_cols)
    padded = count + -count % SUBS
    which = iota((padded, slots), 0)
    seeds = jnp.zeros((padded, slots), jnp.int32)
    for k in range(count):
        seeds = jnp.where(which == k, seeds_ref[:, k : k + 1], seeds)
    live = jnp.where(iota((1, slots), 1) < number_ref[0, 0], 1.0, 0.0)
    live_ref[...] = live
    sampled = (sign_bits(seeds, rows + row_start, cols + col_start) * live).astype(BF16)
    weighted = (dot(sampled, weight_high) + dot(sampled, weight_low)) * live
    row_hot, col_hot = one_hots(cells, block_rows, block_cols)
    parts = pieces(weighted)
    stack = [
        (row_hot * part[k : k + 1].astype(F32)).astype(BF16) for k in range(count) for part in parts
    ]
    spread = lax.dot_general(
        jnp.concatenate(stack, 0), col_hot, (((1,), (1,)), ((), ())), preferred_element_type=F32
    )
    observed = []
    for k in range(count):
        base = 2 * k * block_rows
        high, low = (spread[base + i * block_rows : base + (i + 1) * block_rows] for i in range(2))
        observed.append(low + high)
        obs_ref[k] = observed[k]

    d, cx, cy = d_in[...], cx_in[...], cy_in[...]
    d_ref[...], cx_ref[...], cy_ref[...] = d, cx, cy
    tail = slice(block_rows - SUBS, block_rows)
    last = slice(block_cols - LANES, block_cols)

    sub = iota((SUBS, block_cols), 0)
    rows_next_ref[:SUBS] = cx[tail]
    rows_next_ref[SUBS : 2 * SUBS] = jnp.where(sub >= 4, d[tail], roll(cy[tail], -4, 0))
    for k in range(0, count, 2):
        tile = observed[k][tail]
        if k + 1 < count:
            tile = jnp.where(sub >= 5, tile, roll(observed[k + 1][tail], -3, 0))
        rows_next_ref[(2 + k // 2) * SUBS : (3 + k // 2) * SUBS] = tile

    lane = iota((block_rows, LANES), 1)
    side = jnp.where(lane >= LANES - 5, cy[:, last], roll(d[:, last], -5, 1))
    side = jnp.where(lane >= LANES - 9, side, roll(cx[:, last], -9, 1))
    for k in range(count):
        edge = LANES - 13 - 3 * k
        side = jnp.where(lane >= edge, side, roll(observed[k][:, last], edge, 1))
    cols_next_ref[...] = compact(side, side_width(count))

    lane = iota((SUBS, LANES), 1)
    corner = d[tail, last]
    for i, value in enumerate([cx, cy] + observed):
        edge = LANES - HALO * (i + 1)
        corner = jnp.where(lane >= edge, corner, roll(value[tail, last], edge, 1))
    diag_next_ref[...] = corner

    rows_back_ref[...] = jnp.where(
        sub == 0, cx[:SUBS], jnp.where(sub == 1, roll(d[:SUBS], 1, 0), roll(cy[:SUBS], 2, 0))
    )
    lane = iota((block_rows, LANES), 1)
    back = jnp.where(lane == LANES - 1, roll(cy[:, :LANES], -1, 1), roll(d[:, :LANES], -2, 1))
    back = jnp.where(lane >= LANES - 2, back, roll(cx[:, :LANES], -3, 1))
    cols_back_ref[...] = compact(back, BACK_WIDTH)


TOP = 2 * SUBS


def probes_kernel(seeds_ref, probes_ref):
    count, tiles, wide_rows, _ = probes_ref.shape
    block_rows, block_cols = wide_rows - 2 * TOP, (tiles - 1) * LANES
    row_start = lax.axis_index("gx") * block_rows
    col_start = lax.axis_index("gy") * block_cols
    rows_total = lax.axis_size("gx") * block_rows
    cols_total = lax.axis_size("gy") * block_cols
    row_ids = row_start - TOP + iota((wide_rows, LANES), 0)
    row_ids = jnp.where(row_ids < 0, row_ids + rows_total, row_ids)
    row_ids = jnp.where(row_ids >= rows_total, row_ids - rows_total, row_ids)
    for j in range(tiles):
        col_ids = iota((1, LANES), 1)
        if j == tiles - 1:
            col_ids = jnp.where(col_ids < LANES // 2, col_ids + block_cols, col_ids - LANES)
        else:
            col_ids = col_ids + j * LANES
        col_ids = col_start + col_ids
        col_ids = jnp.where(col_ids < 0, col_ids + cols_total, col_ids)
        col_ids = jnp.where(col_ids >= cols_total, col_ids - cols_total, col_ids)
        for k in range(count):
            probes_ref[k, j] = sign_bits(seeds_ref[:, k : k + 1], row_ids, col_ids)


def side_step(tiles, steps):
    lane = iota(tiles[0].shape, 1)
    turned = [roll(tile, -steps, 1) for tile in tiles]
    if steps > 0:
        return [
            jnp.where(lane == LANES - 1, turned[(j + 1) % len(tiles)], turned[j])
            for j in range(len(tiles))
        ]
    return [jnp.where(lane == 0, turned[j - 1], turned[j]) for j in range(len(tiles))]


def image_kernel(
    live_ref, cells_ref, high_ref, low_ref, d_ref, cx_ref, cy_ref, obs_ref,
    above_ref, left_ref, corner_ref, below_ref, right_ref, probes_ref,
    image_ref, sums_ref, fix_ref,
    centre, cx_wide, cy_wide, cy_before, seen, once, image,
):
    count, block_rows, block_cols = obs_ref.shape
    tiles, _, _ = centre.shape
    side = tiles - 1
    own = slice(TOP, TOP + block_rows)
    over, under = slice(TOP - SUBS, TOP), slice(TOP + block_rows, TOP + block_rows + SUBS)
    left = expand(left_ref[...], block_rows, side_width(count))
    right = expand(right_ref[...], block_rows, BACK_WIDTH)
    corner = corner_ref[...]
    above = above_ref[SUBS : 2 * SUBS]
    below = below_ref[...]
    lane = iota((block_rows, LANES), 1)
    sub, tile_lane = iota((SUBS, LANES), 0), iota((SUBS, LANES), 1)
    nothing = jnp.zeros((SUBS, LANES), F32)

    def lanes_of(j):
        return slice(j * LANES, (j + 1) * LANES)

    for target, block, top, bottom, left_steps, right_steps, corner_steps in (
        (centre, d_ref, above, roll(below, -1, 0), 5, 2, 0),
        (cx_wide, cx_ref, above_ref[:SUBS], below, 9, 3, HALO),
        (cy_wide, cy_ref, roll(above, 4, 0), roll(below, -2, 0), 0, 1, 2 * HALO),
    ):
        for j in range(side):
            target[j, own] = block[:, lanes_of(j)]
            target[j, over] = top[:, lanes_of(j)]
            target[j, under] = bottom[:, lanes_of(j)]
        near = roll(left, left_steps, 1) if left_steps else left
        near = jnp.where(lane >= LANES - HALO, near, 0.0)
        target[side, own] = jnp.where(lane == 0, roll(right, right_steps, 1), near)
        tile = roll(corner, corner_steps, 1) if corner_steps else corner
        target[side, over] = jnp.where(tile_lane >= LANES - HALO, tile, 0.0)
        target[side, under] = nothing
    for k in range(count):
        tile = above_ref[(2 + k // 2) * SUBS : (3 + k // 2) * SUBS]
        tile = roll(tile, 3, 0) if k % 2 else tile
        for j in range(side):
            seen[k, j, own] = obs_ref[k, :, lanes_of(j)]
            seen[k, j, over] = jnp.where(sub >= SUBS - 3, tile[:, lanes_of(j)], 0.0)
        seen[k, side, own] = jnp.where(lane >= LANES - 3, roll(left, 13 + 3 * k, 1), 0.0)
        tile = roll(corner, HALO * (3 + k), 1)
        seen[k, side, over] = jnp.where((tile_lane >= LANES - 3) & (sub >= SUBS - 3), tile, 0.0)

    def rows_at(start, steps=0):
        return pl.ds(start + steps, SUBS)

    def prepare(i, carry):
        start = i * SUBS
        here = rows_at(start)
        cy = [cy_wide[j, here] for j in range(tiles)]
        cy_left = side_step(cy, -1)
        for j in range(tiles):
            cy_before[j, here] = cy_left[j]
            cx_pair = cx_wide[j, here] + cx_wide[j, rows_at(start, -1)]
            centre[j, here] = centre[j, here] + cx_pair + (cy[j] + cy_left[j])
        return carry

    def stencil(field, k, start, coefs):
        here = rows_at(start)
        v = [field[k, j, here] for j in range(tiles)]
        ahead, behind = side_step(v, 1), side_step(v, -1)
        result = []
        for j in range(tiles):
            middle, cx, cx_up, cy, cy_left = coefs[j]
            result.append(
                middle * v[j]
                - cx * field[k, j, rows_at(start, 1)]
                - cx_up * field[k, j, rows_at(start, -1)]
                - cy * ahead[j]
                - cy_left * behind[j]
            )
        return result, v

    def coefs_at(start):
        here = rows_at(start)
        return [
            (
                centre[j, here],
                cx_wide[j, here],
                cx_wide[j, rows_at(start, -1)],
                cy_wide[j, here],
                cy_before[j, here],
            )
            for j in range(tiles)
        ]

    def first(i, carry):
        start = i * SUBS
        coefs = coefs_at(start)
        for k in range(count):
            result, _ = stencil(probes_ref, k, start, coefs)
            for j in range(tiles):
                once[k, j, rows_at(start)] = result[j]
        return carry

    def second(i, carry):
        start = i * SUBS
        coefs = coefs_at(start)
        for k in range(count):
            result, _ = stencil(once, k, start, coefs)
            for j in range(tiles):
                image[k, j, rows_at(start)] = result[j] + seen[k, j, rows_at(start)]
        return carry

    def products(start):
        coefs = coefs_at(start)
        terms = []
        for k in range(count):
            applied, q = stencil(image, k, start, coefs)
            for j in range(tiles):
                terms.append(probes_ref[k, j, rows_at(start)] * q[j])
                terms.append(q[j] * q[j])
                terms.append(applied[j] * applied[j])
        return terms

    def third(i, carry):
        start = i * SUBS
        return tuple(a + b for a, b in zip(carry, products(start)))

    def loop(low, high, step, carry):
        for i in range(low, high):
            carry = step(i, carry)
        return carry

    lead, steps = TOP // SUBS, block_rows // SUBS
    loop(lead - 1, lead + steps + 1, prepare, 0)
    loop(lead - 1, lead + steps + 1, first, 0)
    loop(lead - 1, lead + steps, second, 0)
    edge = [
        jnp.where(sub < SUBS - 2, a, b)
        for a, b in zip(products(TOP + block_rows - SUBS), products(TOP - SUBS))
    ]
    lines = loop(lead, lead + steps - 1, third, tuple(edge))

    slots = cells_ref.shape[1]
    cells = cells_ref[...]
    row_hot, col_hot = one_hots(cells, block_rows, block_cols)
    live = live_ref[...]
    stack, first_miss, second_miss = [], [], []
    for k in range(count):
        whole = jnp.concatenate([image[k, j, own] for j in range(side)], 1)
        image_ref[k] = whole
        stack.extend(pieces(whole))
        low = TOP + block_rows
        first_miss.append(
            cx_ref[block_rows - 1 : block_rows, 0:1]
            * (probes_ref[k, side, low : low + 1, LANES - 1 :] - probes_ref[k, 0, low : low + 1, 0:1])
        )
        second_miss.append(
            cy_ref[0:1, block_cols - 1 : block_cols]
            * (probes_ref[k, side, TOP - 1 : TOP, 0:1] - probes_ref[k, side, TOP : TOP + 1, 0:1])
        )
    found = dot(jnp.concatenate(stack, 0), col_hot)
    sampled = []
    for k in range(count):
        base = 2 * k * block_rows
        high, low = (found[base + i * block_rows : base + (i + 1) * block_rows] for i in range(2))
        sampled.append(jnp.sum((low + high) * row_hot, 0, keepdims=True) * live)
    first_hot = jnp.where(cells == (block_rows - 1) * block_cols, live, 0.0)
    second_hot = jnp.where(cells == block_cols - 1, live, 0.0)
    spare = -(count + 2) % SUBS
    points = sampled + [first_hot, second_hot] + [jnp.zeros((spare, slots), F32)] * (spare > 0)
    points = jnp.concatenate(points, 0)
    high, low = pieces(points)
    weighted = dot(high, high_ref[...]) + (dot(low, high_ref[...]) + dot(high, low_ref[...]))

    def total(value):
        return jnp.sum(value, 1, keepdims=True)

    with_points = total(points * weighted)
    with_first = total(points * weighted[count : count + 1] + weighted * first_hot)
    with_second = total(points * weighted[count + 1 : count + 2] + weighted * second_hot)
    out_lane = iota((1, LANES), 1)
    row = jnp.zeros((1, LANES), F32)
    fix = jnp.zeros((1, LANES), F32)
    for k in range(count):
        one, two = first_miss[k], second_miss[k]
        values = []
        for i in range(3):
            line = [jnp.sum(lines[3 * (k * tiles + j) + i], 0, keepdims=True) for j in range(tiles)]
            line[side - 1] = jnp.where(out_lane < LANES - 2, line[side - 1], line[side])
            values.append(total(sum(line[:side])))
        values[2] = values[2] + with_points[k : k + 1]
        values.append(one * with_first[k : k + 1])
        values.append(two * with_second[k : k + 1])
        values.append(one * one * with_points[count : count + 1])
        values.append(two * two * with_points[count + 1 : count + 2])
        values.append(one * two * with_first[count + 1 : count + 2])
        for i, value in enumerate(values):
            row = jnp.where(out_lane == i * count + k, value, row)
        fix = jnp.where(out_lane == k, one, jnp.where(out_lane == count + k, two, fix))
    row = jnp.where(out_lane == 8 * count, cy_ref[0:1, block_cols - 1 : block_cols], row)
    row = jnp.where(out_lane == 8 * count + 1, cx_ref[block_rows - 1 : block_rows, 0:1], row)
    sums_ref[...] = jnp.broadcast_to(row[None], sums_ref.shape)
    fix_ref[...] = fix


def finish_kernel(sums_ref, probes_ref, image_ref, fix_ref, solution_ref, trace_ref):
    count, block_rows, block_cols = image_ref.shape
    across = lax.axis_size("gy")
    devices = sums_ref.shape[0]
    rows = jnp.sum(sums_ref[...], 1)
    member = iota((devices, 1), 0)
    place = lax.rem(member, across)
    lower = roll(rows, -across, 0)
    lower = jnp.where(place == 0, roll(lower, 1 - across, 0), roll(lower, 1, 0))
    upper = roll(rows, across, 0)
    upper = jnp.where(place == across - 1, roll(upper, across - 1, 0), roll(upper, -1, 0))
    one = lower[:, 8 * count : 8 * count + 1]
    two = upper[:, 8 * count + 1 : 8 * count + 2]
    part = [roll(rows, -i * count, 1) if i else rows for i in range(8)]
    third = part[2] + one * (part[3] + one * part[5] + two * part[7]) + two * (part[4] + two * part[6])

    cells_total = float(block_rows * block_cols * devices)
    first = jnp.sum(part[0], 0, keepdims=True)
    second = jnp.sum(part[1], 0, keepdims=True)
    third = jnp.sum(third, 0, keepdims=True)
    step = cells_total / first
    growth = step * step * second * (1.0 / cells_total)
    ratio = growth - 1.0
    bend = step * step * step * third * (1.0 / cells_total) - growth * growth
    next_step = step * ratio / bend
    on_probe = step + next_step * growth
    on_image = step * next_step
    used = iota(first.shape, 1) < count
    trace = jnp.where(used, step + next_step * ratio, 0.0)
    trace_ref[...] = jnp.sum(trace, 1, keepdims=True) * (cells_total / count)

    mine = member == lax.axis_index("gx") * across + lax.axis_index("gy")
    fix = fix_ref[...]
    change = on_image * fix * jnp.sum(jnp.where(mine, one, 0.0), 0, keepdims=True)
    other = on_image * roll(fix, -count, 1) * jnp.sum(jnp.where(mine, two, 0.0), 0, keepdims=True)
    tile_sub, tile_lane = iota((SUBS, LANES), 0), iota((SUBS, LANES), 1)
    low_left = (tile_sub == SUBS - 1) & (tile_lane == 0)
    high_right = (tile_sub == 0) & (tile_lane == LANES - 1)
    tail = slice(block_rows - SUBS, block_rows)
    last = slice(block_cols - LANES, block_cols)
    for k in range(count):
        here = slice(k, k + 1)
        probe = [
            probes_ref[k, j, TOP : TOP + block_rows] for j in range(block_cols // LANES)
        ]
        value = on_probe[:, here] * jnp.concatenate(probe, 1) - on_image[:, here] * image_ref[k]
        solution_ref[k] = value
        solution_ref[k, tail, :LANES] = solution_ref[k, tail, :LANES] - jnp.where(
            low_left, change[:, here], 0.0
        )
        solution_ref[k, :SUBS, last] = solution_ref[k, :SUBS, last] - jnp.where(
            high_right, other[:, here], 0.0
        )


def per_device(
    probe_seeds, damping, coupling_x, coupling_y, sensor_count, sensor_cells, obs_weight
):
    block_rows, block_cols = damping.shape
    count = probe_seeds.shape[0]
    slots = obs_weight.shape[-1]
    wide = (block_cols // LANES + 1, block_rows + 2 * TOP, LANES)
    devices = lax.axis_size("gx") * lax.axis_size("gy")
    full = jax.ShapeDtypeStruct

    def call(kernel, args, outs, scratch=(), scalars=0):
        return pl.pallas_call(
            kernel,
            out_shape=outs,
            in_specs=[SMEM] * scalars + [VMEM] * (len(args) - scalars),
            out_specs=[VMEM] * len(outs),
            scratch_shapes=scratch,
        )(*args)

    def space(*shape):
        return pltpu.VMEM(shape, F32)

    block = space(block_rows, block_cols)
    blocks = space(count, block_rows, block_cols)
    seeds = probe_seeds.reshape(1, count)
    outs = call(
        start_kernel,
        (
            sensor_count,
            seeds,
            sensor_cells.reshape(1, slots),
            obs_weight.reshape(slots, slots),
            damping,
            coupling_x,
            coupling_y,
        ),
        [
            pltpu.VMEM((1, count), jnp.int32),
            pltpu.VMEM((1, slots), jnp.int32),
            pltpu.VMEM((slots, slots), BF16),
            pltpu.VMEM((slots, slots), BF16),
            block,
            block,
            block,
            blocks,
            space(1, slots),
            space(SUBS * (2 + (count + 1) // 2), block_cols),
            space(compact_rows(block_rows, side_width(count)), LANES),
            space(SUBS, LANES),
            space(SUBS, block_cols),
            space(compact_rows(block_rows, BACK_WIDTH), LANES),
        ],
        scalars=1,
    )
    seeds, cells, high, low, *coefs, observed, live = on_chip(*outs[:9])
    rows_next, cols_next, diag_next, rows_back, cols_back = outs[9:]
    above = shifted(rows_next, "gx", 1)
    corner = shifted_both(diag_next)
    left = shifted(cols_next, "gy", 1)
    below = shifted(rows_back, "gx", -1)
    right = shifted(cols_back, "gy", -1)

    probes, = on_chip(
        *call(probes_kernel, (seeds,), [space(count, *wide)])
    )
    image, sums, fix = call(
        image_kernel,
        (
            live,
            cells,
            high,
            low,
            *coefs,
            observed,
            *on_chip(above, left, corner, below, right),
            probes,
        ),
        [blocks, space(devices, 1, LANES), space(1, LANES)],
        [space(*wide)] * 4 + [space(count, *wide)] * 3,
    )
    sums = lax.all_to_all(sums, ("gx", "gy"), 0, 0, tiled=True)
    solved, trace = call(
        finish_kernel,
        (*on_chip(sums), probes, *on_chip(image, fix)),
        [full((count, block_rows, block_cols), F32), full((1, 1), F32)],
    )
    return solved, trace[0, 0]


def solution(mesh):
    placed = (
        P(),
        P("gx", "gy"),
        P("gx", "gy"),
        P("gx", "gy"),
        P("gx", "gy"),
        P("gx", "gy", None),
        P("gx", "gy", None, None),
    )

    return jax.shard_map(
        per_device,
        mesh=mesh,
        in_specs=placed,
        out_specs=(P(None, "gx", "gy"), P()),
        check_vma=False,
    )
```

```python
import jax
import jax.numpy as jnp
from jax import lax
from jax.experimental import pallas as pl
from jax.experimental.pallas import tpu as pltpu
from jax.sharding import PartitionSpec as P


LANES = 128
SUBS = 8
F32 = jnp.float32
BF16 = jnp.bfloat16
SMEM = pl.BlockSpec(memory_space=pltpu.SMEM)
VMEM = pl.BlockSpec(memory_space=pltpu.VMEM)


def swapped(value, axis, odd_first):
    count = lax.axis_size(axis)
    pairs = [(i, (i + (1 if i % 2 == odd_first else -1)) % count) for i in range(count)]
    return lax.ppermute(value, axis, pairs)


def shifted_both(value):
    down, across = lax.axis_size("gx"), lax.axis_size("gy")
    pairs = [
        (x * across + y, (x + 1) % down * across + (y + 1) % across)
        for x in range(down)
        for y in range(across)
    ]
    return lax.ppermute(value, ("gx", "gy"), pairs)


def on_chip(*values):
    return tuple(pltpu.with_memory_space_constraint(value, pltpu.VMEM) for value in values)


def sign_bits(seeds, row_ids, col_ids):
    mixed = seeds * 668265261 + row_ids * 374761393 + col_ids * 1103515245
    mixed = (mixed ^ ((mixed >> 16) & 65535)) * 73244475
    mixed = (mixed ^ ((mixed >> 16) & 65535)) * 73244475
    mixed = mixed ^ ((mixed >> 16) & 65535)
    return (2 * ((mixed >> 7) & 1) - 1).astype(F32)


def iota(shape, dim):
    return lax.broadcasted_iota(jnp.int32, shape, dim)


def roll(value, steps, dim):
    return pltpu.roll(value, steps % value.shape[dim], dim)


def pieces(value):
    high = value.astype(BF16)
    return high, (value - high.astype(F32)).astype(BF16)


def dot(left, right):
    return jnp.dot(left, right, preferred_element_type=F32)


def split_cells(cells, block_cols):
    rows = jnp.floor((cells.astype(F32) + 0.5) * (1.0 / block_cols)).astype(jnp.int32)
    return rows, cells - rows * block_cols


def one_hots(cells, block_rows, block_cols):
    rows, cols = split_cells(cells, block_cols)
    slots = cells.shape[1]
    row_hot = jnp.where(iota((block_rows, slots), 0) == rows, 1.0, 0.0)
    col_hot = jnp.where(iota((block_cols, slots), 0) == cols, 1.0, 0.0).astype(BF16)
    return row_hot, col_hot


def compact(value, width):
    per = LANES // width
    tiles = value.shape[0] // SUBS
    lane = iota((SUBS, LANES), 1)
    packed = []
    for start in range(0, tiles, per):
        total = value[start * SUBS : (start + 1) * SUBS]
        for i in range(1, min(per, tiles - start)):
            tile = value[(start + i) * SUBS : (start + i + 1) * SUBS]
            total = jnp.where(lane < LANES - width * i, roll(tile, -width * i, 1), total)
        packed.append(total)
    return packed[0] if len(packed) == 1 else jnp.concatenate(packed, 0)


def expand(packed, rows, width):
    per = LANES // width
    tiles = []
    for i in range(rows // SUBS):
        start = i // per * SUBS
        tile = packed[start : start + SUBS]
        tiles.append(roll(tile, width * (i % per), 1) if i % per else tile)
    return jnp.concatenate(tiles, 0)


def compact_rows(rows, width):
    per = LANES // width
    return SUBS * (-(-rows // SUBS // per))


def side_width(count):
    width = 1
    while width < 13 + 3 * count:
        width *= 2
    return width


BACK_WIDTH = 8
HALO = 5


def start_kernel(
    number_ref, seeds_ref, cells_in, weight_in, d_in, cx_in, cy_in,
    seeds_out, cells_ref, high_ref, low_ref, d_ref, cx_ref, cy_ref, obs_ref, live_ref,
    rows_next_ref, cols_next_ref, diag_next_ref, rows_back_ref, cols_back_ref,
):
    count, block_rows, block_cols = obs_ref.shape
    row_start = lax.axis_index("gx") * block_rows
    col_start = lax.axis_index("gy") * block_cols
    slots = cells_in.shape[1]
    cells = cells_in[...]
    seeds_out[...] = seeds_ref[...]
    cells_ref[...] = cells
    weight_high, weight_low = pieces(weight_in[...])
    high_ref[...], low_ref[...] = weight_high, weight_low
    rows, cols = split_cells(cells, block_cols)
    padded = count + -count % SUBS
    which = iota((padded, slots), 0)
    seeds = jnp.zeros((padded, slots), jnp.int32)
    for k in range(count):
        seeds = jnp.where(which == k, seeds_ref[:, k : k + 1], seeds)
    live = jnp.where(iota((1, slots), 1) < number_ref[0, 0], 1.0, 0.0)
    live_ref[...] = live
    sampled = (sign_bits(seeds, rows + row_start, cols + col_start) * live).astype(BF16)
    weighted = (dot(sampled, weight_high) + dot(sampled, weight_low)) * live
    row_hot, col_hot = one_hots(cells, block_rows, block_cols)
    parts = pieces(weighted)
    stack = [
        (row_hot * part[k : k + 1].astype(F32)).astype(BF16) for k in range(count) for part in parts
    ]
    spread = lax.dot_general(
        jnp.concatenate(stack, 0), col_hot, (((1,), (1,)), ((), ())), preferred_element_type=F32
    )
    observed = []
    for k in range(count):
        base = 2 * k * block_rows
        high, low = (spread[base + i * block_rows : base + (i + 1) * block_rows] for i in range(2))
        observed.append(low + high)
        obs_ref[k] = observed[k]

    d, cx, cy = d_in[...], cx_in[...], cy_in[...]
    d_ref[...], cx_ref[...], cy_ref[...] = d, cx, cy
    tail = slice(block_rows - SUBS, block_rows)
    last = slice(block_cols - LANES, block_cols)

    sub = iota((SUBS, block_cols), 0)
    onward = [cx[tail], jnp.where(sub >= 4, d[tail], roll(cy[tail], -4, 0))]
    for k in range(0, count, 2):
        tile = observed[k][tail]
        if k + 1 < count:
            tile = jnp.where(sub >= 5, tile, roll(observed[k + 1][tail], -3, 0))
        onward.append(tile)

    lane = iota((block_rows, LANES), 1)
    side = jnp.where(lane >= LANES - 5, cy[:, last], roll(d[:, last], -5, 1))
    side = jnp.where(lane >= LANES - 9, side, roll(cx[:, last], -9, 1))
    for k in range(count):
        edge = LANES - 13 - 3 * k
        side = jnp.where(lane >= edge, side, roll(observed[k][:, last], edge, 1))
    cols_onward = compact(side, side_width(count))

    lane = iota((SUBS, LANES), 1)
    corner = d[tail, last]
    for i, value in enumerate([cx, cy] + observed):
        edge = LANES - HALO * (i + 1)
        corner = jnp.where(lane >= edge, corner, roll(value[tail, last], edge, 1))
    diag_next_ref[...] = corner

    back = jnp.where(
        sub == 0, cx[:SUBS], jnp.where(sub == 1, roll(d[:SUBS], 1, 0), roll(cy[:SUBS], 2, 0))
    )
    odd = lax.rem(lax.axis_index("gx"), 2) == 1
    rows_next_ref[:SUBS] = jnp.where(odd, onward[0], back)
    rows_back_ref[:SUBS] = jnp.where(odd, back, onward[0])
    for i in range(1, len(onward)):
        rows_next_ref[i * SUBS : (i + 1) * SUBS] = onward[i]
        rows_back_ref[i * SUBS : (i + 1) * SUBS] = onward[i]
    lane = iota((block_rows, LANES), 1)
    back = jnp.where(lane == LANES - 1, roll(cy[:, :LANES], -1, 1), roll(d[:, :LANES], -2, 1))
    back = jnp.where(lane >= LANES - 2, back, roll(cx[:, :LANES], -3, 1))
    cols_back = compact(back, BACK_WIDTH)
    size = cols_back.shape[0]
    odd = lax.rem(lax.axis_index("gy"), 2) == 1
    cols_next_ref[...] = cols_onward
    cols_back_ref[...] = cols_onward
    cols_next_ref[:size] = jnp.where(odd, cols_onward[:size], cols_back)
    cols_back_ref[:size] = jnp.where(odd, cols_back, cols_onward[:size])


TOP = 2 * SUBS


def probes_kernel(seeds_ref, probes_ref):
    count, tiles, wide_rows, _ = probes_ref.shape
    block_rows, block_cols = wide_rows - 2 * TOP, (tiles - 1) * LANES
    row_start = lax.axis_index("gx") * block_rows
    col_start = lax.axis_index("gy") * block_cols
    rows_total = lax.axis_size("gx") * block_rows
    cols_total = lax.axis_size("gy") * block_cols
    row_ids = row_start - TOP + iota((wide_rows, LANES), 0)
    row_ids = jnp.where(row_ids < 0, row_ids + rows_total, row_ids)
    row_ids = jnp.where(row_ids >= rows_total, row_ids - rows_total, row_ids)
    for j in range(tiles):
        col_ids = iota((1, LANES), 1)
        if j == tiles - 1:
            col_ids = jnp.where(col_ids < LANES // 2, col_ids + block_cols, col_ids - LANES)
        else:
            col_ids = col_ids + j * LANES
        col_ids = col_start + col_ids
        col_ids = jnp.where(col_ids < 0, col_ids + cols_total, col_ids)
        col_ids = jnp.where(col_ids >= cols_total, col_ids - cols_total, col_ids)
        for k in range(count):
            probes_ref[k, j] = sign_bits(seeds_ref[:, k : k + 1], row_ids, col_ids)


def side_step(tiles, steps):
    lane = iota(tiles[0].shape, 1)
    turned = [roll(tile, -steps, 1) for tile in tiles]
    if steps > 0:
        return [
            jnp.where(lane == LANES - 1, turned[(j + 1) % len(tiles)], turned[j])
            for j in range(len(tiles))
        ]
    return [jnp.where(lane == 0, turned[j - 1], turned[j]) for j in range(len(tiles))]


def image_kernel(
    live_ref, cells_ref, high_ref, low_ref, d_ref, cx_ref, cy_ref, obs_ref,
    rows_a_ref, rows_b_ref, cols_a_ref, cols_b_ref, corner_ref, probes_ref,
    image_ref, sums_ref, fix_ref,
    centre, cx_wide, cy_wide, cy_before, seen, once, image,
):
    count, block_rows, block_cols = obs_ref.shape
    tiles, _, _ = centre.shape
    side = tiles - 1
    own = slice(TOP, TOP + block_rows)
    over, under = slice(TOP - SUBS, TOP), slice(TOP + block_rows, TOP + block_rows + SUBS)
    odd = lax.rem(lax.axis_index("gy"), 2) == 1
    cols_a, cols_b = cols_a_ref[...], cols_b_ref[...]
    left = expand(jnp.where(odd, cols_a, cols_b), block_rows, side_width(count))
    right = expand(jnp.where(odd, cols_b, cols_a), block_rows, BACK_WIDTH)
    corner = corner_ref[...]
    odd = lax.rem(lax.axis_index("gx"), 2) == 1
    above_ref = jnp.where(odd, rows_a_ref[...], rows_b_ref[...])
    above = above_ref[SUBS : 2 * SUBS]
    below = jnp.where(odd, rows_b_ref[:SUBS], rows_a_ref[:SUBS])
    lane = iota((block_rows, LANES), 1)
    sub, tile_lane = iota((SUBS, LANES), 0), iota((SUBS, LANES), 1)
    nothing = jnp.zeros((SUBS, LANES), F32)

    def lanes_of(j):
        return slice(j * LANES, (j + 1) * LANES)

    for target, block, top, bottom, left_steps, right_steps, corner_steps in (
        (centre, d_ref, above, roll(below, -1, 0), 5, 2, 0),
        (cx_wide, cx_ref, above_ref[:SUBS], below, 9, 3, HALO),
        (cy_wide, cy_ref, roll(above, 4, 0), roll(below, -2, 0), 0, 1, 2 * HALO),
    ):
        for j in range(side):
            target[j, own] = block[:, lanes_of(j)]
            target[j, over] = top[:, lanes_of(j)]
            target[j, under] = bottom[:, lanes_of(j)]
        near = roll(left, left_steps, 1) if left_steps else left
        near = jnp.where(lane >= LANES - HALO, near, 0.0)
        target[side, own] = jnp.where(lane == 0, roll(right, right_steps, 1), near)
        tile = roll(corner, corner_steps, 1) if corner_steps else corner
        target[side, over] = jnp.where(tile_lane >= LANES - HALO, tile, 0.0)
        target[side, under] = nothing
    for k in range(count):
        tile = above_ref[(2 + k // 2) * SUBS : (3 + k // 2) * SUBS]
        tile = roll(tile, 3, 0) if k % 2 else tile
        for j in range(side):
            seen[k, j, own] = obs_ref[k, :, lanes_of(j)]
            seen[k, j, over] = jnp.where(sub >= SUBS - 3, tile[:, lanes_of(j)], 0.0)
        seen[k, side, own] = jnp.where(lane >= LANES - 3, roll(left, 13 + 3 * k, 1), 0.0)
        tile = roll(corner, HALO * (3 + k), 1)
        seen[k, side, over] = jnp.where((tile_lane >= LANES - 3) & (sub >= SUBS - 3), tile, 0.0)

    def rows_at(start, steps=0):
        return pl.ds(start + steps, SUBS)

    def prepare(i, carry):
        start = i * SUBS
        here = rows_at(start)
        cy = [cy_wide[j, here] for j in range(tiles)]
        cy_left = side_step(cy, -1)
        for j in range(tiles):
            cy_before[j, here] = cy_left[j]
            cx_pair = cx_wide[j, here] + cx_wide[j, rows_at(start, -1)]
            centre[j, here] = centre[j, here] + cx_pair + (cy[j] + cy_left[j])
        return carry

    def stencil(field, k, start, coefs):
        here = rows_at(start)
        v = [field[k, j, here] for j in range(tiles)]
        ahead, behind = side_step(v, 1), side_step(v, -1)
        result = []
        for j in range(tiles):
            middle, cx, cx_up, cy, cy_left = coefs[j]
            result.append(
                middle * v[j]
                - cx * field[k, j, rows_at(start, 1)]
                - cx_up * field[k, j, rows_at(start, -1)]
                - cy * ahead[j]
                - cy_left * behind[j]
            )
        return result, v

    def coefs_at(start):
        here = rows_at(start)
        return [
            (
                centre[j, here],
                cx_wide[j, here],
                cx_wide[j, rows_at(start, -1)],
                cy_wide[j, here],
                cy_before[j, here],
            )
            for j in range(tiles)
        ]

    def first(i, carry):
        start = i * SUBS
        coefs = coefs_at(start)
        for k in range(count):
            result, _ = stencil(probes_ref, k, start, coefs)
            for j in range(tiles):
                once[k, j, rows_at(start)] = result[j]
        return carry

    def second(i, carry):
        start = i * SUBS
        coefs = coefs_at(start)
        for k in range(count):
            result, _ = stencil(once, k, start, coefs)
            for j in range(tiles):
                image[k, j, rows_at(start)] = result[j] + seen[k, j, rows_at(start)]
        return carry

    def products(start):
        coefs = coefs_at(start)
        terms = []
        for k in range(count):
            applied, q = stencil(image, k, start, coefs)
            for j in range(tiles):
                terms.append(probes_ref[k, j, rows_at(start)] * q[j])
                terms.append(q[j] * q[j])
                terms.append(applied[j] * applied[j])
        return terms

    def third(i, carry):
        start = i * SUBS
        return tuple(a + b for a, b in zip(carry, products(start)))

    def loop(low, high, step, carry):
        for i in range(low, high):
            carry = step(i, carry)
        return carry

    lead, steps = TOP // SUBS, block_rows // SUBS
    loop(lead - 1, lead + steps + 1, prepare, 0)
    loop(lead - 1, lead + steps + 1, first, 0)
    loop(lead - 1, lead + steps, second, 0)
    edge = [
        jnp.where(sub < SUBS - 2, a, b)
        for a, b in zip(products(TOP + block_rows - SUBS), products(TOP - SUBS))
    ]
    lines = loop(lead, lead + steps - 1, third, tuple(edge))

    slots = cells_ref.shape[1]
    cells = cells_ref[...]
    row_hot, col_hot = one_hots(cells, block_rows, block_cols)
    live = live_ref[...]
    stack, first_miss, second_miss = [], [], []
    for k in range(count):
        whole = jnp.concatenate([image[k, j, own] for j in range(side)], 1)
        image_ref[k] = whole
        stack.extend(pieces(whole))
        low = TOP + block_rows
        first_miss.append(
            cx_ref[block_rows - 1 : block_rows, 0:1]
            * (probes_ref[k, side, low : low + 1, LANES - 1 :] - probes_ref[k, 0, low : low + 1, 0:1])
        )
        second_miss.append(
            cy_ref[0:1, block_cols - 1 : block_cols]
            * (probes_ref[k, side, TOP - 1 : TOP, 0:1] - probes_ref[k, side, TOP : TOP + 1, 0:1])
        )
    found = dot(jnp.concatenate(stack, 0), col_hot)
    sampled = []
    for k in range(count):
        base = 2 * k * block_rows
        high, low = (found[base + i * block_rows : base + (i + 1) * block_rows] for i in range(2))
        sampled.append(jnp.sum((low + high) * row_hot, 0, keepdims=True) * live)
    first_hot = jnp.where(cells == (block_rows - 1) * block_cols, live, 0.0)
    second_hot = jnp.where(cells == block_cols - 1, live, 0.0)
    spare = -(count + 2) % SUBS
    points = sampled + [first_hot, second_hot] + [jnp.zeros((spare, slots), F32)] * (spare > 0)
    points = jnp.concatenate(points, 0)
    high, low = pieces(points)
    weighted = dot(high, high_ref[...]) + (dot(low, high_ref[...]) + dot(high, low_ref[...]))

    def total(value):
        return jnp.sum(value, 1, keepdims=True)

    with_points = total(points * weighted)
    with_first = total(points * weighted[count : count + 1] + weighted * first_hot)
    with_second = total(points * weighted[count + 1 : count + 2] + weighted * second_hot)
    out_lane = iota((1, LANES), 1)
    row = jnp.zeros((1, LANES), F32)
    fix = jnp.zeros((1, LANES), F32)
    for k in range(count):
        one, two = first_miss[k], second_miss[k]
        values = []
        for i in range(3):
            line = [jnp.sum(lines[3 * (k * tiles + j) + i], 0, keepdims=True) for j in range(tiles)]
            line[side - 1] = jnp.where(out_lane < LANES - 2, line[side - 1], line[side])
            values.append(total(sum(line[:side])))
        values[2] = values[2] + with_points[k : k + 1]
        values.append(one * with_first[k : k + 1])
        values.append(two * with_second[k : k + 1])
        values.append(one * one * with_points[count : count + 1])
        values.append(two * two * with_points[count + 1 : count + 2])
        values.append(one * two * with_first[count + 1 : count + 2])
        for i, value in enumerate(values):
            row = jnp.where(out_lane == i * count + k, value, row)
        fix = jnp.where(out_lane == k, one, jnp.where(out_lane == count + k, two, fix))
    row = jnp.where(out_lane == 8 * count, cy_ref[0:1, block_cols - 1 : block_cols], row)
    row = jnp.where(out_lane == 8 * count + 1, cx_ref[block_rows - 1 : block_rows, 0:1], row)
    sums_ref[...] = jnp.broadcast_to(row[None], sums_ref.shape)
    fix_ref[...] = fix


def finish_kernel(sums_ref, probes_ref, image_ref, fix_ref, solution_ref, trace_ref):
    count, block_rows, block_cols = image_ref.shape
    across = lax.axis_size("gy")
    devices = sums_ref.shape[0]
    rows = jnp.sum(sums_ref[...], 1)
    member = iota((devices, 1), 0)
    place = lax.rem(member, across)
    lower = roll(rows, -across, 0)
    lower = jnp.where(place == 0, roll(lower, 1 - across, 0), roll(lower, 1, 0))
    upper = roll(rows, across, 0)
    upper = jnp.where(place == across - 1, roll(upper, across - 1, 0), roll(upper, -1, 0))
    one = lower[:, 8 * count : 8 * count + 1]
    two = upper[:, 8 * count + 1 : 8 * count + 2]
    part = [roll(rows, -i * count, 1) if i else rows for i in range(8)]
    third = part[2] + one * (part[3] + one * part[5] + two * part[7]) + two * (part[4] + two * part[6])

    cells_total = float(block_rows * block_cols * devices)
    first = jnp.sum(part[0], 0, keepdims=True)
    second = jnp.sum(part[1], 0, keepdims=True)
    third = jnp.sum(third, 0, keepdims=True)
    step = cells_total / first
    growth = step * step * second * (1.0 / cells_total)
    ratio = growth - 1.0
    bend = step * step * step * third * (1.0 / cells_total) - growth * growth
    next_step = step * ratio / bend
    on_probe = step + next_step * growth
    on_image = step * next_step
    used = iota(first.shape, 1) < count
    trace = jnp.where(used, step + next_step * ratio, 0.0)
    trace_ref[...] = jnp.sum(trace, 1, keepdims=True) * (cells_total / count)

    mine = member == lax.axis_index("gx") * across + lax.axis_index("gy")
    fix = fix_ref[...]
    change = on_image * fix * jnp.sum(jnp.where(mine, one, 0.0), 0, keepdims=True)
    other = on_image * roll(fix, -count, 1) * jnp.sum(jnp.where(mine, two, 0.0), 0, keepdims=True)
    tile_sub, tile_lane = iota((SUBS, LANES), 0), iota((SUBS, LANES), 1)
    low_left = (tile_sub == SUBS - 1) & (tile_lane == 0)
    high_right = (tile_sub == 0) & (tile_lane == LANES - 1)
    tail = slice(block_rows - SUBS, block_rows)
    last = slice(block_cols - LANES, block_cols)
    for k in range(count):
        here = slice(k, k + 1)
        probe = [
            probes_ref[k, j, TOP : TOP + block_rows] for j in range(block_cols // LANES)
        ]
        value = on_probe[:, here] * jnp.concatenate(probe, 1) - on_image[:, here] * image_ref[k]
        solution_ref[k] = value
        solution_ref[k, tail, :LANES] = solution_ref[k, tail, :LANES] - jnp.where(
            low_left, change[:, here], 0.0
        )
        solution_ref[k, :SUBS, last] = solution_ref[k, :SUBS, last] - jnp.where(
            high_right, other[:, here], 0.0
        )


def per_device(
    probe_seeds, damping, coupling_x, coupling_y, sensor_count, sensor_cells, obs_weight
):
    block_rows, block_cols = damping.shape
    count = probe_seeds.shape[0]
    slots = obs_weight.shape[-1]
    wide = (block_cols // LANES + 1, block_rows + 2 * TOP, LANES)
    devices = lax.axis_size("gx") * lax.axis_size("gy")
    full = jax.ShapeDtypeStruct

    def call(kernel, args, outs, scratch=(), scalars=0):
        return pl.pallas_call(
            kernel,
            out_shape=outs,
            in_specs=[SMEM] * scalars + [VMEM] * (len(args) - scalars),
            out_specs=[VMEM] * len(outs),
            scratch_shapes=scratch,
        )(*args)

    def space(*shape):
        return pltpu.VMEM(shape, F32)

    block = space(block_rows, block_cols)
    blocks = space(count, block_rows, block_cols)
    seeds = probe_seeds.reshape(1, count)
    outs = call(
        start_kernel,
        (
            sensor_count,
            seeds,
            sensor_cells.reshape(1, slots),
            obs_weight.reshape(slots, slots),
            damping,
            coupling_x,
            coupling_y,
        ),
        [
            pltpu.VMEM((1, count), jnp.int32),
            pltpu.VMEM((1, slots), jnp.int32),
            pltpu.VMEM((slots, slots), BF16),
            pltpu.VMEM((slots, slots), BF16),
            block,
            block,
            block,
            blocks,
            space(1, slots),
            space(SUBS * (2 + (count + 1) // 2), block_cols),
            space(compact_rows(block_rows, side_width(count)), LANES),
            space(SUBS, LANES),
            space(SUBS * (2 + (count + 1) // 2), block_cols),
            space(compact_rows(block_rows, side_width(count)), LANES),
        ],
        scalars=1,
    )
    seeds, cells, high, low, *coefs, observed, live = on_chip(*outs[:9])
    rows_next, cols_next, diag_next, rows_back, cols_back = outs[9:]
    rows_b = swapped(rows_next, "gx", 1)
    rows_a = swapped(rows_back, "gx", 0)
    corner = shifted_both(diag_next)
    cols_b = swapped(cols_next, "gy", 1)
    cols_a = swapped(cols_back, "gy", 0)

    probes, = on_chip(
        *call(probes_kernel, (seeds,), [space(count, *wide)])
    )
    image, sums, fix = call(
        image_kernel,
        (
            live,
            cells,
            high,
            low,
            *coefs,
            observed,
            *on_chip(rows_a, rows_b, cols_a, cols_b, corner),
            probes,
        ),
        [blocks, space(devices, 1, LANES), space(1, LANES)],
        [space(*wide)] * 4 + [space(count, *wide)] * 3,
    )
    sums = lax.all_to_all(sums, ("gx", "gy"), 0, 0, tiled=True)
    solved, trace = call(
        finish_kernel,
        (*on_chip(sums), probes, *on_chip(image, fix)),
        [full((count, block_rows, block_cols), F32), full((1, 1), F32)],
    )
    return solved, trace[0, 0]


def solution(mesh):
    placed = (
        P(),
        P("gx", "gy"),
        P("gx", "gy"),
        P("gx", "gy"),
        P("gx", "gy"),
        P("gx", "gy", None),
        P("gx", "gy", None, None),
    )

    return jax.shard_map(
        per_device,
        mesh=mesh,
        in_specs=placed,
        out_specs=(P(None, "gx", "gy"), P()),
        check_vma=False,
    )
```

```python
import jax
import jax.numpy as jnp
from jax import lax
from jax.experimental import pallas as pl
from jax.experimental.pallas import tpu as pltpu
from jax.sharding import PartitionSpec as P


LANES = 128
SUBS = 8
F32 = jnp.float32
BF16 = jnp.bfloat16
SMEM = pl.BlockSpec(memory_space=pltpu.SMEM)
VMEM = pl.BlockSpec(memory_space=pltpu.VMEM)


def swapped(value, axis, odd_first):
    count = lax.axis_size(axis)
    pairs = [(i, (i + (1 if i % 2 == odd_first else -1)) % count) for i in range(count)]
    return lax.ppermute(value, axis, pairs)


def shifted_both(value):
    down, across = lax.axis_size("gx"), lax.axis_size("gy")
    pairs = [
        (x * across + y, (x + 1) % down * across + (y + 1) % across)
        for x in range(down)
        for y in range(across)
    ]
    return lax.ppermute(value, ("gx", "gy"), pairs)


def on_chip(*values):
    return tuple(pltpu.with_memory_space_constraint(value, pltpu.VMEM) for value in values)


def sign_bits(seeds, row_ids, col_ids):
    mixed = seeds * 668265261 + row_ids * 374761393 + col_ids * 1103515245
    mixed = (mixed ^ ((mixed >> 16) & 65535)) * 73244475
    mixed = (mixed ^ ((mixed >> 16) & 65535)) * 73244475
    mixed = mixed ^ ((mixed >> 16) & 65535)
    return (2 * ((mixed >> 7) & 1) - 1).astype(F32)


def iota(shape, dim):
    return lax.broadcasted_iota(jnp.int32, shape, dim)


def roll(value, steps, dim):
    return pltpu.roll(value, steps % value.shape[dim], dim)


def pieces(value):
    high = value.astype(BF16)
    return high, (value - high.astype(F32)).astype(BF16)


def dot(left, right):
    return jnp.dot(left, right, preferred_element_type=F32)


def split_cells(cells, block_cols):
    rows = jnp.floor((cells.astype(F32) + 0.5) * (1.0 / block_cols)).astype(jnp.int32)
    return rows, cells - rows * block_cols


def one_hots(cells, block_rows, block_cols):
    rows, cols = split_cells(cells, block_cols)
    slots = cells.shape[1]
    row_hot = jnp.where(iota((block_rows, slots), 0) == rows, 1.0, 0.0)
    col_hot = jnp.where(iota((block_cols, slots), 0) == cols, 1.0, 0.0).astype(BF16)
    return row_hot, col_hot


def compact(value, width):
    per = LANES // width
    tiles = value.shape[0] // SUBS
    lane = iota((SUBS, LANES), 1)
    packed = []
    for start in range(0, tiles, per):
        total = value[start * SUBS : (start + 1) * SUBS]
        for i in range(1, min(per, tiles - start)):
            tile = value[(start + i) * SUBS : (start + i + 1) * SUBS]
            total = jnp.where(lane < LANES - width * i, roll(tile, -width * i, 1), total)
        packed.append(total)
    return packed[0] if len(packed) == 1 else jnp.concatenate(packed, 0)


def expand(packed, rows, width):
    per = LANES // width
    tiles = []
    for i in range(rows // SUBS):
        start = i // per * SUBS
        tile = packed[start : start + SUBS]
        tiles.append(roll(tile, width * (i % per), 1) if i % per else tile)
    return jnp.concatenate(tiles, 0)


def compact_rows(rows, width):
    per = LANES // width
    return SUBS * (-(-rows // SUBS // per))


def side_width(count):
    width = 1
    while width < 13 + 3 * count:
        width *= 2
    return width


BACK_WIDTH = 8
HALO = 5


def start_kernel(
    number_ref, seeds_ref, cells_in, weight_in, d_in, cx_in, cy_in,
    seeds_out, cells_ref, high_ref, low_ref, d_ref, cx_ref, cy_ref, obs_ref, live_ref,
    rows_next_ref, cols_next_ref, diag_next_ref, rows_back_ref, cols_back_ref,
):
    count, block_rows, block_cols = obs_ref.shape
    row_start = lax.axis_index("gx") * block_rows
    col_start = lax.axis_index("gy") * block_cols
    slots = cells_in.shape[1]
    cells = cells_in[...]
    seeds_out[...] = seeds_ref[...]
    cells_ref[...] = cells
    weight_high, weight_low = pieces(weight_in[...])
    high_ref[...], low_ref[...] = weight_high, weight_low
    rows, cols = split_cells(cells, block_cols)
    padded = count + -count % SUBS
    which = iota((padded, slots), 0)
    seeds = jnp.zeros((padded, slots), jnp.int32)
    for k in range(count):
        seeds = jnp.where(which == k, seeds_ref[:, k : k + 1], seeds)
    live = jnp.where(iota((1, slots), 1) < number_ref[0, 0], 1.0, 0.0)
    live_ref[...] = live
    sampled = (sign_bits(seeds, rows + row_start, cols + col_start) * live).astype(BF16)
    weighted = (dot(sampled, weight_high) + dot(sampled, weight_low)) * live
    row_hot, col_hot = one_hots(cells, block_rows, block_cols)
    parts = pieces(weighted)
    stack = [
        (row_hot * part[k : k + 1].astype(F32)).astype(BF16) for k in range(count) for part in parts
    ]
    spread = lax.dot_general(
        jnp.concatenate(stack, 0), col_hot, (((1,), (1,)), ((), ())), preferred_element_type=F32
    )
    observed = []
    for k in range(count):
        base = 2 * k * block_rows
        high, low = (spread[base + i * block_rows : base + (i + 1) * block_rows] for i in range(2))
        observed.append(low + high)
        obs_ref[k] = observed[k]

    d, cx, cy = d_in[...], cx_in[...], cy_in[...]
    d_ref[...], cx_ref[...], cy_ref[...] = d, cx, cy
    tail = slice(block_rows - SUBS, block_rows)
    last = slice(block_cols - LANES, block_cols)

    sub = iota((SUBS, block_cols), 0)
    onward = [cx[tail], jnp.where(sub >= 4, d[tail], roll(cy[tail], -4, 0))]
    for k in range(0, count, 2):
        tile = observed[k][tail]
        if k + 1 < count:
            tile = jnp.where(sub >= 5, tile, roll(observed[k + 1][tail], -3, 0))
        onward.append(tile)

    lane = iota((block_rows, LANES), 1)
    side = jnp.where(lane >= LANES - 5, cy[:, last], roll(d[:, last], -5, 1))
    side = jnp.where(lane >= LANES - 9, side, roll(cx[:, last], -9, 1))
    for k in range(count):
        edge = LANES - 13 - 3 * k
        side = jnp.where(lane >= edge, side, roll(observed[k][:, last], edge, 1))
    cols_onward = compact(side, side_width(count))

    lane = iota((SUBS, LANES), 1)
    corner = d[tail, last]
    for i, value in enumerate([cx, cy] + observed):
        edge = LANES - HALO * (i + 1)
        corner = jnp.where(lane >= edge, corner, roll(value[tail, last], edge, 1))
    diag_next_ref[...] = corner

    back = jnp.where(
        sub == 0, cx[:SUBS], jnp.where(sub == 1, roll(d[:SUBS], 1, 0), roll(cy[:SUBS], 2, 0))
    )
    odd = lax.rem(lax.axis_index("gx"), 2) == 1
    rows_next_ref[:SUBS] = jnp.where(odd, onward[0], back)
    rows_back_ref[:SUBS] = jnp.where(odd, back, onward[0])
    for i in range(1, len(onward)):
        rows_next_ref[i * SUBS : (i + 1) * SUBS] = onward[i]
        rows_back_ref[i * SUBS : (i + 1) * SUBS] = onward[i]
    lane = iota((block_rows, LANES), 1)
    back = jnp.where(lane == LANES - 1, roll(cy[:, :LANES], -1, 1), roll(d[:, :LANES], -2, 1))
    back = jnp.where(lane >= LANES - 2, back, roll(cx[:, :LANES], -3, 1))
    cols_back = compact(back, BACK_WIDTH)
    size = cols_back.shape[0]
    odd = lax.rem(lax.axis_index("gy"), 2) == 1
    cols_next_ref[...] = cols_onward
    cols_back_ref[...] = cols_onward
    cols_next_ref[:size] = jnp.where(odd, cols_onward[:size], cols_back)
    cols_back_ref[:size] = jnp.where(odd, cols_back, cols_onward[:size])


TOP = 2 * SUBS


def probes_kernel(seeds_ref, cells_ref, probes_ref, row_hot_ref, col_hot_ref):
    count, tiles, wide_rows, _ = probes_ref.shape
    block_rows, block_cols = wide_rows - 2 * TOP, (tiles - 1) * LANES
    row_start = lax.axis_index("gx") * block_rows
    col_start = lax.axis_index("gy") * block_cols
    rows_total = lax.axis_size("gx") * block_rows
    cols_total = lax.axis_size("gy") * block_cols
    row_ids = row_start - TOP + iota((wide_rows, LANES), 0)
    row_ids = jnp.where(row_ids < 0, row_ids + rows_total, row_ids)
    row_ids = jnp.where(row_ids >= rows_total, row_ids - rows_total, row_ids)
    for j in range(tiles):
        col_ids = iota((1, LANES), 1)
        if j == tiles - 1:
            col_ids = jnp.where(col_ids < LANES // 2, col_ids + block_cols, col_ids - LANES)
        else:
            col_ids = col_ids + j * LANES
        col_ids = col_start + col_ids
        col_ids = jnp.where(col_ids < 0, col_ids + cols_total, col_ids)
        col_ids = jnp.where(col_ids >= cols_total, col_ids - cols_total, col_ids)
        for k in range(count):
            probes_ref[k, j] = sign_bits(seeds_ref[:, k : k + 1], row_ids, col_ids)
    row_hot, col_hot = one_hots(cells_ref[...], block_rows, block_cols)
    row_hot_ref[...], col_hot_ref[...] = row_hot, col_hot


def side_step(tiles, steps):
    lane = iota(tiles[0].shape, 1)
    turned = [roll(tile, -steps, 1) for tile in tiles]
    if steps > 0:
        return [
            jnp.where(lane == LANES - 1, turned[(j + 1) % len(tiles)], turned[j])
            for j in range(len(tiles))
        ]
    return [jnp.where(lane == 0, turned[j - 1], turned[j]) for j in range(len(tiles))]


def image_kernel(
    live_ref, cells_ref, high_ref, low_ref, d_ref, cx_ref, cy_ref, obs_ref,
    rows_a_ref, rows_b_ref, cols_a_ref, cols_b_ref, corner_ref, probes_ref,
    row_hot_ref, col_hot_ref, image_ref, sums_ref, fix_ref,
    centre, cx_wide, cy_wide, cy_before, seen, once, image,
):
    count, block_rows, block_cols = obs_ref.shape
    tiles, _, _ = centre.shape
    side = tiles - 1
    own = slice(TOP, TOP + block_rows)
    over, under = slice(TOP - SUBS, TOP), slice(TOP + block_rows, TOP + block_rows + SUBS)
    odd = lax.rem(lax.axis_index("gy"), 2) == 1
    cols_a, cols_b = cols_a_ref[...], cols_b_ref[...]
    left = expand(jnp.where(odd, cols_a, cols_b), block_rows, side_width(count))
    right = expand(jnp.where(odd, cols_b, cols_a), block_rows, BACK_WIDTH)
    corner = corner_ref[...]
    odd = lax.rem(lax.axis_index("gx"), 2) == 1
    above_ref = jnp.where(odd, rows_a_ref[...], rows_b_ref[...])
    above = above_ref[SUBS : 2 * SUBS]
    below = jnp.where(odd, rows_b_ref[:SUBS], rows_a_ref[:SUBS])
    lane = iota((block_rows, LANES), 1)
    sub, tile_lane = iota((SUBS, LANES), 0), iota((SUBS, LANES), 1)
    nothing = jnp.zeros((SUBS, LANES), F32)

    def lanes_of(j):
        return slice(j * LANES, (j + 1) * LANES)

    for target, block, top, bottom, left_steps, right_steps, corner_steps in (
        (centre, d_ref, above, roll(below, -1, 0), 5, 2, 0),
        (cx_wide, cx_ref, above_ref[:SUBS], below, 9, 3, HALO),
        (cy_wide, cy_ref, roll(above, 4, 0), roll(below, -2, 0), 0, 1, 2 * HALO),
    ):
        for j in range(side):
            target[j, own] = block[:, lanes_of(j)]
            target[j, over] = top[:, lanes_of(j)]
            target[j, under] = bottom[:, lanes_of(j)]
        near = roll(left, left_steps, 1) if left_steps else left
        near = jnp.where(lane >= LANES - HALO, near, 0.0)
        target[side, own] = jnp.where(lane == 0, roll(right, right_steps, 1), near)
        tile = roll(corner, corner_steps, 1) if corner_steps else corner
        target[side, over] = jnp.where(tile_lane >= LANES - HALO, tile, 0.0)
        target[side, under] = nothing
    for k in range(count):
        tile = above_ref[(2 + k // 2) * SUBS : (3 + k // 2) * SUBS]
        tile = roll(tile, 3, 0) if k % 2 else tile
        for j in range(side):
            seen[k, j, over] = jnp.where(sub >= SUBS - 3, tile[:, lanes_of(j)], 0.0)
        seen[k, side, own] = jnp.where(lane >= LANES - 3, roll(left, 13 + 3 * k, 1), 0.0)
        tile = roll(corner, HALO * (3 + k), 1)
        seen[k, side, over] = jnp.where((tile_lane >= LANES - 3) & (sub >= SUBS - 3), tile, 0.0)

    def rows_at(start, steps=0):
        return pl.ds(start + steps, SUBS)

    def prepare(i, carry):
        start = i * SUBS
        here = rows_at(start)
        cy = [cy_wide[j, here] for j in range(tiles)]
        cy_left = side_step(cy, -1)
        for j in range(tiles):
            cy_before[j, here] = cy_left[j]
            cx_pair = cx_wide[j, here] + cx_wide[j, rows_at(start, -1)]
            centre[j, here] = centre[j, here] + cx_pair + (cy[j] + cy_left[j])
        return carry

    def stencil(field, k, start, coefs):
        here = rows_at(start)
        v = [field[k, j, here] for j in range(tiles)]
        ahead, behind = side_step(v, 1), side_step(v, -1)
        result = []
        for j in range(tiles):
            middle, cx, cx_up, cy, cy_left = coefs[j]
            result.append(
                middle * v[j]
                - cx * field[k, j, rows_at(start, 1)]
                - cx_up * field[k, j, rows_at(start, -1)]
                - cy * ahead[j]
                - cy_left * behind[j]
            )
        return result, v

    def coefs_at(start):
        here = rows_at(start)
        return [
            (
                centre[j, here],
                cx_wide[j, here],
                cx_wide[j, rows_at(start, -1)],
                cy_wide[j, here],
                cy_before[j, here],
            )
            for j in range(tiles)
        ]

    def first(i, carry):
        start = i * SUBS
        coefs = coefs_at(start)
        for k in range(count):
            result, _ = stencil(probes_ref, k, start, coefs)
            for j in range(tiles):
                once[k, j, rows_at(start)] = result[j]
        return carry

    def second(i, carry):
        start = i * SUBS
        coefs = coefs_at(start)
        for k in range(count):
            result, _ = stencil(once, k, start, coefs)
            for j in range(tiles):
                if j == side or start < TOP:
                    added = seen[k, j, rows_at(start)]
                else:
                    added = obs_ref[k, rows_at(start, -TOP), lanes_of(j)]
                image[k, j, rows_at(start)] = result[j] + added
        return carry

    def products(start):
        coefs = coefs_at(start)
        terms = []
        for k in range(count):
            applied, q = stencil(image, k, start, coefs)
            for j in range(tiles):
                terms.append(probes_ref[k, j, rows_at(start)] * q[j])
                terms.append(q[j] * q[j])
                terms.append(applied[j] * applied[j])
        return terms

    def third(i, carry):
        start = i * SUBS
        return tuple(a + b for a, b in zip(carry, products(start)))

    def loop(low, high, step, carry):
        for i in range(low, high):
            carry = step(i, carry)
        return carry

    lead, steps = TOP // SUBS, block_rows // SUBS
    loop(lead - 1, lead + steps + 1, prepare, 0)
    loop(lead - 1, lead + steps + 1, first, 0)
    loop(lead - 1, lead + steps, second, 0)
    edge = [
        jnp.where(sub < SUBS - 2, a, b)
        for a, b in zip(products(TOP + block_rows - SUBS), products(TOP - SUBS))
    ]
    lines = loop(lead, lead + steps - 1, third, tuple(edge))

    slots = cells_ref.shape[1]
    cells = cells_ref[...]
    row_hot, col_hot = row_hot_ref[...], col_hot_ref[...]
    live = live_ref[...]
    stack, first_miss, second_miss = [], [], []
    for k in range(count):
        whole = jnp.concatenate([image[k, j, own] for j in range(side)], 1)
        image_ref[k] = whole
        stack.extend(pieces(whole))
        low = TOP + block_rows
        first_miss.append(
            cx_ref[block_rows - 1 : block_rows, 0:1]
            * (probes_ref[k, side, low : low + 1, LANES - 1 :] - probes_ref[k, 0, low : low + 1, 0:1])
        )
        second_miss.append(
            cy_ref[0:1, block_cols - 1 : block_cols]
            * (probes_ref[k, side, TOP - 1 : TOP, 0:1] - probes_ref[k, side, TOP : TOP + 1, 0:1])
        )
    found = dot(jnp.concatenate(stack, 0), col_hot)
    sampled = []
    for k in range(count):
        base = 2 * k * block_rows
        high, low = (found[base + i * block_rows : base + (i + 1) * block_rows] for i in range(2))
        sampled.append(jnp.sum((low + high) * row_hot, 0, keepdims=True) * live)
    first_hot = jnp.where(cells == (block_rows - 1) * block_cols, live, 0.0)
    second_hot = jnp.where(cells == block_cols - 1, live, 0.0)
    spare = -(count + 2) % SUBS
    points = sampled + [first_hot, second_hot] + [jnp.zeros((spare, slots), F32)] * (spare > 0)
    points = jnp.concatenate(points, 0)
    high, low = pieces(points)
    weighted = dot(high, high_ref[...]) + (dot(low, high_ref[...]) + dot(high, low_ref[...]))

    def total(value):
        return jnp.sum(value, 1, keepdims=True)

    with_points = total(points * weighted)
    with_first = total(points * weighted[count : count + 1] + weighted * first_hot)
    with_second = total(points * weighted[count + 1 : count + 2] + weighted * second_hot)
    out_lane = iota((1, LANES), 1)
    row = jnp.zeros((1, LANES), F32)
    fix = jnp.zeros((1, LANES), F32)
    for k in range(count):
        one, two = first_miss[k], second_miss[k]
        values = []
        for i in range(3):
            line = [jnp.sum(lines[3 * (k * tiles + j) + i], 0, keepdims=True) for j in range(tiles)]
            line[side - 1] = jnp.where(out_lane < LANES - 2, line[side - 1], line[side])
            values.append(total(sum(line[:side])))
        values[2] = values[2] + with_points[k : k + 1]
        values.append(one * with_first[k : k + 1])
        values.append(two * with_second[k : k + 1])
        values.append(one * one * with_points[count : count + 1])
        values.append(two * two * with_points[count + 1 : count + 2])
        values.append(one * two * with_first[count + 1 : count + 2])
        for i, value in enumerate(values):
            row = jnp.where(out_lane == i * count + k, value, row)
        fix = jnp.where(out_lane == k, one, jnp.where(out_lane == count + k, two, fix))
    row = jnp.where(out_lane == 8 * count, cy_ref[0:1, block_cols - 1 : block_cols], row)
    row = jnp.where(out_lane == 8 * count + 1, cx_ref[block_rows - 1 : block_rows, 0:1], row)
    sums_ref[...] = jnp.broadcast_to(row[None], sums_ref.shape)
    fix_ref[...] = fix


def finish_kernel(sums_ref, probes_ref, image_ref, fix_ref, solution_ref, trace_ref):
    count, block_rows, block_cols = image_ref.shape
    across = lax.axis_size("gy")
    devices = sums_ref.shape[0]
    rows = jnp.sum(sums_ref[...], 1)
    member = iota((devices, 1), 0)
    place = lax.rem(member, across)
    lower = roll(rows, -across, 0)
    lower = jnp.where(place == 0, roll(lower, 1 - across, 0), roll(lower, 1, 0))
    upper = roll(rows, across, 0)
    upper = jnp.where(place == across - 1, roll(upper, across - 1, 0), roll(upper, -1, 0))
    one = lower[:, 8 * count : 8 * count + 1]
    two = upper[:, 8 * count + 1 : 8 * count + 2]
    part = [roll(rows, -i * count, 1) if i else rows for i in range(8)]
    third = part[2] + one * (part[3] + one * part[5] + two * part[7]) + two * (part[4] + two * part[6])

    cells_total = float(block_rows * block_cols * devices)
    first = jnp.sum(part[0], 0, keepdims=True)
    second = jnp.sum(part[1], 0, keepdims=True)
    third = jnp.sum(third, 0, keepdims=True)
    step = cells_total / first
    growth = step * step * second * (1.0 / cells_total)
    ratio = growth - 1.0
    bend = step * step * step * third * (1.0 / cells_total) - growth * growth
    next_step = step * ratio / bend
    on_probe = step + next_step * growth
    on_image = step * next_step
    used = iota(first.shape, 1) < count
    trace = jnp.where(used, step + next_step * ratio, 0.0)
    trace_ref[...] = jnp.sum(trace, 1, keepdims=True) * (cells_total / count)

    mine = member == lax.axis_index("gx") * across + lax.axis_index("gy")
    fix = fix_ref[...]
    change = on_image * fix * jnp.sum(jnp.where(mine, one, 0.0), 0, keepdims=True)
    other = on_image * roll(fix, -count, 1) * jnp.sum(jnp.where(mine, two, 0.0), 0, keepdims=True)
    tile_sub, tile_lane = iota((SUBS, LANES), 0), iota((SUBS, LANES), 1)
    low_left = (tile_sub == SUBS - 1) & (tile_lane == 0)
    high_right = (tile_sub == 0) & (tile_lane == LANES - 1)
    tail = slice(block_rows - SUBS, block_rows)
    last = slice(block_cols - LANES, block_cols)
    for k in range(count):
        here = slice(k, k + 1)
        probe = [
            probes_ref[k, j, TOP : TOP + block_rows] for j in range(block_cols // LANES)
        ]
        value = on_probe[:, here] * jnp.concatenate(probe, 1) - on_image[:, here] * image_ref[k]
        solution_ref[k] = value
        solution_ref[k, tail, :LANES] = solution_ref[k, tail, :LANES] - jnp.where(
            low_left, change[:, here], 0.0
        )
        solution_ref[k, :SUBS, last] = solution_ref[k, :SUBS, last] - jnp.where(
            high_right, other[:, here], 0.0
        )


def per_device(
    probe_seeds, damping, coupling_x, coupling_y, sensor_count, sensor_cells, obs_weight
):
    block_rows, block_cols = damping.shape
    count = probe_seeds.shape[0]
    slots = obs_weight.shape[-1]
    wide = (block_cols // LANES + 1, block_rows + 2 * TOP, LANES)
    devices = lax.axis_size("gx") * lax.axis_size("gy")
    full = jax.ShapeDtypeStruct

    def call(kernel, args, outs, scratch=(), scalars=0):
        return pl.pallas_call(
            kernel,
            out_shape=outs,
            in_specs=[SMEM] * scalars + [VMEM] * (len(args) - scalars),
            out_specs=[VMEM] * len(outs),
            scratch_shapes=scratch,
        )(*args)

    def space(*shape):
        return pltpu.VMEM(shape, F32)

    block = space(block_rows, block_cols)
    blocks = space(count, block_rows, block_cols)
    seeds = probe_seeds.reshape(1, count)
    outs = call(
        start_kernel,
        (
            sensor_count,
            seeds,
            sensor_cells.reshape(1, slots),
            obs_weight.reshape(slots, slots),
            damping,
            coupling_x,
            coupling_y,
        ),
        [
            pltpu.VMEM((1, count), jnp.int32),
            pltpu.VMEM((1, slots), jnp.int32),
            pltpu.VMEM((slots, slots), BF16),
            pltpu.VMEM((slots, slots), BF16),
            block,
            block,
            block,
            blocks,
            space(1, slots),
            space(SUBS * (2 + (count + 1) // 2), block_cols),
            space(compact_rows(block_rows, side_width(count)), LANES),
            space(SUBS, LANES),
            space(SUBS * (2 + (count + 1) // 2), block_cols),
            space(compact_rows(block_rows, side_width(count)), LANES),
        ],
        scalars=1,
    )
    seeds, cells, high, low, *coefs, observed, live = on_chip(*outs[:9])
    rows_next, cols_next, diag_next, rows_back, cols_back = outs[9:]
    rows_b = swapped(rows_next, "gx", 1)
    rows_a = swapped(rows_back, "gx", 0)
    corner = shifted_both(diag_next)
    cols_b = swapped(cols_next, "gy", 1)
    cols_a = swapped(cols_back, "gy", 0)

    probes, row_hot, col_hot = on_chip(
        *call(
            probes_kernel,
            (seeds, cells),
            [space(count, *wide), space(block_rows, slots), pltpu.VMEM((block_cols, slots), BF16)],
        )
    )
    image, sums, fix = call(
        image_kernel,
        (
            live,
            cells,
            high,
            low,
            *coefs,
            observed,
            *on_chip(rows_a, rows_b, cols_a, cols_b, corner),
            probes,
            row_hot,
            col_hot,
        ),
        [blocks, space(devices, 1, LANES), space(1, LANES)],
        [space(*wide)] * 4 + [space(count, *wide)] * 3,
    )
    sums = lax.all_to_all(sums, ("gx", "gy"), 0, 0, tiled=True)
    solved, trace = call(
        finish_kernel,
        (*on_chip(sums), probes, *on_chip(image, fix)),
        [full((count, block_rows, block_cols), F32), full((1, 1), F32)],
    )
    return solved, trace[0, 0]


def solution(mesh):
    placed = (
        P(),
        P("gx", "gy"),
        P("gx", "gy"),
        P("gx", "gy"),
        P("gx", "gy"),
        P("gx", "gy", None),
        P("gx", "gy", None, None),
    )

    return jax.shard_map(
        per_device,
        mesh=mesh,
        in_specs=placed,
        out_specs=(P(None, "gx", "gy"), P()),
        check_vma=False,
    )
```
